32 devices in a mesh: grp: 8 (over y, x, core), seq: 4 (over z).
Axes of the slice: x: 2, y: 2, z: 4, core: 2. Of those that a mesh axis runs over, the one named last changes fastest.
Arguments:
- tokens: bfloat16 [16, 16, 256, 384], P(None, 'grp', 'seq'), may hold values from -6 to 6
- cotangent: bfloat16 [16, 16, 256, 384], P(None, 'grp', 'seq'), may hold values from -6 to 6
- condition: float32 [16, 16, 384], P(None, 'grp'), may hold values from -6 to 6
- mask_flags: int32 [16, 16], P(None, 'grp'), may hold values 0 or 1
- noise_levels: int32 [16, 16], P(None, 'grp'), may hold values from 0 to 63
- level_table: float32 [64, 384], replicated, may hold values from -6 to 6
- ada_weight: bfloat16 [384, 2304], replicated, may hold values from -0.3125 to 0.3125
- ada_bias: float32 [2304], replicated, may hold values from -3 to 3
- qkv_weight: bfloat16 [384, 1152], replicated, may hold values from -0.3125 to 0.3125
- query_value_bias: float32 [768], replicated, may hold values from -1.75 to 1.75
- output_weight: bfloat16 [384, 384], replicated, may hold values from -1.25 to 1.25
- output_bias: float32 [384], replicated, may hold values from -1.75 to 1.75
- up_weight: bfloat16 [384, 1536], replicated, may hold values from -0.3125 to 0.3125
- up_bias: float32 [1536], replicated, may hold values from -1.75 to 1.75
- down_weight: bfloat16 [1536, 384], replicated, may hold values from -0.15625 to 0.15625
- down_bias: float32 [384], replicated, may hold values from -1.75 to 1.75
Outputs:
- layer_out: bfloat16 [16, 16, 256, 384], P(None, 'grp', 'seq')
- grad_tokens: bfloat16 [16, 16, 256, 384], P(None, 'grp', 'seq')
- grad_condition: float32 [16, 16, 384], P(None, 'grp')
- grad_level_table: float32 [64, 384], replicated
- grad_ada_weight: float32 [384, 2304], replicated
- grad_ada_bias: float32 [2304], replicated
- grad_qkv_weight: float32 [384, 1152], replicated
- grad_query_value_bias: float32 [768], replicated
- grad_output_weight: float32 [384, 384], replicated
- grad_output_bias: float32 [384], replicated
- grad_up_weight: float32 [384, 1536], replicated
- grad_up_bias: float32 [1536], replicated
- grad_down_weight: float32 [1536, 384], replicated
- grad_down_bias: float32 [384], replicated
The draws below stay inside these ranges and needn't reach their ends.
Inputs may be any that keep to these rules, and one draw needn't show every extreme that they name: `mask_flags`: 1 marks an image of which only the first 128 rows are kept patches; its other rows are padding.
All inputs are finite; a program needn't handle non-finite values. No bound on the sum of `mask_flags` on one device may be relied on, other than what follows from the above.
Results may differ from the reference program's by a relative error of at most 0.015.
The reference program's roundings to bfloat16 on the way count: a program that leaves them out, or rounds other values in their place, can miss the bound.
Values may be sent and summed in bfloat16 or wider, within the bound.
No kernel may reach another device: no remote copies, remote signals or barrier semaphores. Data moves between devices by JAX's collectives and lax.ppermute only.
A program may use at most 128 MiB of HBM per device.

```python
import math
import jax
import jax.numpy as jnp
import numpy as np
from jax import lax

D = 384
HEADS = 6
HEAD_DIM = 64
FF = 1536
SEQ_LEN = 256
KEEP = 128
LEVELS = 64
MICRO = 16
IMAGES = 16


def set_ends(values, stream_key, low, largest):
    shape = values.shape
    spot = [jax.random.randint(jax.random.fold_in(stream_key, axis), (), 0, shape[axis]) for axis in range(len(shape))]
    values = values.at[tuple(spot)].set(low)
    longest = shape.index(max(shape))
    spot[longest] = (spot[longest] + 1) % shape[longest]
    return values.at[tuple(spot)].set(largest)


def shard_levels(key, dims, cuts, least, largest):
    level = 1.0
    for position, parts in cuts:
        steps = jax.random.uniform(jax.random.fold_in(jax.random.fold_in(key, 6), position), (parts,), jnp.float32, least / len(cuts), largest / len(cuts))
        level = level * jnp.repeat(jnp.exp(steps), dims[position] // parts).reshape((-1,) + (1,) * (len(dims) - 1 - position))
    return level


def rank_table(amount, lean):
    weights = [(1 << 20) // math.isqrt(rank ** lean) + 1 for rank in range(1, amount + 1)]
    spread = 1 + sum(weights) // (1 << 30)
    return np.cumsum(np.array([max(1, weight // spread) for weight in weights]))


def ranked(own_key, dims, number_of, slope):
    listing = rank_table(number_of, slope)
    pick = jax.random.randint(jax.random.fold_in(own_key, 1), dims, 0, int(listing[number_of - 1]))
    standing = jnp.searchsorted(jnp.asarray(listing, jnp.int32), pick, side="right")
    return jax.random.permutation(jax.random.fold_in(own_key, 2), number_of)[standing].astype(jnp.int32)


def scatter_about(key, dims, scale, reach, pieces=(), kind=jnp.bfloat16):
    factor_of = shard_levels(key, dims, pieces, -0.22, 0.18) if pieces else 1.0
    entries = jax.random.normal(key, dims, jnp.float32) * scale * factor_of
    return jnp.minimum(jnp.maximum(entries, -reach), reach).astype(kind)


def setup_inputs(seed: int = 0) -> dict:
    arg_keys = jax.random.split(jax.random.key(seed), 17)
    return {
        "tokens": scatter_about(arg_keys[0], (MICRO, IMAGES, SEQ_LEN, D), 1.0, 6.0, ((1, 8), (2, 4))),
        "cotangent": scatter_about(arg_keys[1], (MICRO, IMAGES, SEQ_LEN, D), 1.0, 6.0, ((1, 8), (2, 4))),
        "condition": scatter_about(arg_keys[2], (MICRO, IMAGES, D), 1.0, 6.0, ((1, 8),), jnp.float32),
        "mask_flags": set_ends((jax.random.randint(arg_keys[3], (MICRO, IMAGES), 0, 2) < 1).astype(jnp.int32), jax.random.fold_in(arg_keys[3], 1), 0, 1),
        "noise_levels": set_ends(ranked(arg_keys[4], (MICRO, IMAGES), LEVELS, 2), jax.random.fold_in(arg_keys[4], 3), 0, LEVELS - 1).astype(jnp.int32),
        "level_table": scatter_about(arg_keys[5], (LEVELS, D), 1.0, 6.0, (), jnp.float32),
        "ada_weight": scatter_about(arg_keys[6], (D, 6 * D), D ** -0.5, 0.3125),
        "ada_bias": scatter_about(arg_keys[7], (6 * D,), 0.5, 3.0, (), jnp.float32),
        "qkv_weight": scatter_about(arg_keys[8], (D, 3 * D), D ** -0.5, 0.3125),
        "query_value_bias": scatter_about(arg_keys[9], (2 * D,), 0.3, 1.75, (), jnp.float32),
        "output_weight": scatter_about(arg_keys[10], (D, D), (D // 16) ** -0.5, 1.25),
        "output_bias": scatter_about(arg_keys[11], (D,), 0.3, 1.75, (), jnp.float32),
        "up_weight": scatter_about(arg_keys[12], (D, FF), D ** -0.5, 0.3125),
        "up_bias": scatter_about(arg_keys[13], (FF,), 0.3, 1.75, (), jnp.float32),
        "down_weight": scatter_about(arg_keys[14], (FF, D), FF ** -0.5, 0.15625),
        "down_bias": scatter_about(arg_keys[15], (D,), 0.3, 1.75, (), jnp.float32),
    }


@jax.custom_vjp
def low(v):
    return lax.optimization_barrier(v.astype(jnp.bfloat16)).astype(jnp.float32)

@jax.custom_vjp
def low_back(v):
    return v

def low_keep(v):
    return (low(v), None)

def low_pass(kept, grad):
    return (grad,)

def back_keep(v):
    return (v, None)

def back_low(kept, grad):
    return (low(grad),)
low.defvjp(low_keep, low_pass)
low_back.defvjp(back_keep, back_low)
highest = lax.Precision.HIGHEST

def layer_norm(values):
    average = lax.optimization_barrier(jnp.mean(values, -1, keepdims=True))
    centered = values - average
    return centered * lax.rsqrt(lax.optimization_barrier(jnp.mean(centered * centered, -1, keepdims=True)) + 1e-06)

def project(values, weight, bias):
    return jnp.einsum('nsd,de->nse', values, weight, precision=highest) + bias

def forward(params, tokens, condition, mask_flags, noise_levels):
    level_table, ada_weight, ada_bias, qkv_weight, query_value_bias, output_weight, output_bias, up_weight, up_bias, down_weight, down_bias = params
    image_count = tokens.shape[0]
    row_ids = jnp.arange(SEQ_LEN, dtype=jnp.int32)
    live_keys = jnp.logical_or(mask_flags[:, None] == 0, row_ids[None, :] < KEEP)
    live_rows = live_keys.astype(tokens.dtype)[..., None]
    cond_full = condition + level_table[noise_levels]
    activated = low(jax.nn.silu(cond_full))
    modulation = jnp.dot(activated, ada_weight, precision=highest) + ada_bias
    shift_one, scale_one, gate_one, shift_two, scale_two, gate_two = jnp.split(modulation[:, None, :], 6, axis=-1)
    in_one = low(layer_norm(tokens) * (1.0 + scale_one) + shift_one)
    zero_bias = jnp.zeros((D,), tokens.dtype)
    bias_full = jnp.concatenate([query_value_bias[:D], zero_bias, query_value_bias[D:]])
    projected = low(low_back(project(in_one, qkv_weight, bias_full)))
    query_heads = projected[..., :D].reshape(image_count, SEQ_LEN, HEADS, HEAD_DIM)
    key_heads = projected[..., D:2 * D].reshape(image_count, SEQ_LEN, HEADS, HEAD_DIM)
    value_heads = projected[..., 2 * D:].reshape(image_count, SEQ_LEN, HEADS, HEAD_DIM)
    raw_scores = jnp.einsum('nqhd,nkhd->nhqk', query_heads, key_heads, precision=highest) * (1.0 / math.sqrt(HEAD_DIM))
    scores = jnp.where(live_keys[:, None, None, :], low_back(raw_scores), -1e+30)
    attn_probs = jax.nn.softmax(scores, axis=-1)
    attended = jnp.einsum('nhqk,nkhd->nqhd', low(attn_probs), value_heads, precision=highest)
    attended = low(low_back(attended.reshape(image_count, SEQ_LEN, D)))
    attn_branch = low_back(project(attended, output_weight, output_bias))
    residual = tokens + live_rows * gate_one * attn_branch
    in_two = low(layer_norm(residual) * (1.0 + scale_two) + shift_two)
    pre_act = low_back(project(in_two, up_weight, up_bias))
    hidden = low(jax.nn.gelu(pre_act, approximate=True))
    ffn_branch = low_back(project(hidden, down_weight, down_bias))
    return residual + live_rows * gate_two * ffn_branch

def reference(tokens, cotangent, condition, mask_flags, noise_levels, level_table, ada_weight, ada_bias, qkv_weight, query_value_bias, output_weight, output_bias, up_weight, up_bias, down_weight, down_bias):
    total_images = MICRO * IMAGES
    block_size = math.gcd(total_images, 16)
    block_count = total_images // block_size
    params = tuple((item.astype(jnp.float32) for item in (level_table, ada_weight, ada_bias, qkv_weight, query_value_bias, output_weight, output_bias, up_weight, up_bias, down_weight, down_bias)))

    def to_blocks(array):
        return array.reshape((block_count, block_size) + array.shape[2:])
    block_inputs = (to_blocks(tokens.astype(jnp.float32)), to_blocks(cotangent.astype(jnp.float32)), to_blocks(condition.astype(jnp.float32)), to_blocks(mask_flags), to_blocks(noise_levels))

    def one_block(carry, block_data):
        block_tokens, block_cot, block_cond, block_flags, block_levels = block_data

        def local_forward(weights, inputs, cond_in):
            return forward(weights, inputs, cond_in, block_flags, block_levels)
        result, pullback = jax.vjp(local_forward, params, block_tokens, block_cond)
        grad_params, grad_inputs, grad_cond = pullback(block_cot)
        carry = jax.tree.map(jnp.add, carry, grad_params)
        return (carry, (result, grad_inputs, grad_cond))
    initial = jax.tree.map(jnp.zeros_like, params)
    sums, (results, grad_inputs, grad_cond) = lax.scan(one_block, initial, block_inputs)
    return (results.reshape(tokens.shape).astype(jnp.bfloat16), grad_inputs.reshape(tokens.shape).astype(jnp.bfloat16), grad_cond.reshape(condition.shape), sums[0], sums[1], sums[2], sums[3], sums[4], sums[5], sums[6], sums[7], sums[8], sums[9], sums[10])
```

```python
import functools
import math

import jax
import jax.numpy as jnp
from jax import lax
from jax.experimental import pallas as pl
from jax.experimental.pallas import tpu as pltpu
from jax.sharding import PartitionSpec as P

D = 384
HEADS = 6
HEAD_DIM = 64
FF = 1536
SEQ_LEN = 256
KEEP = 128
LEVELS = 64
EPSILON = 1e-06
highest = lax.Precision.HIGHEST

UP, DOWN, QKV, OUT, WIDE = 0, FF, 2 * FF, 2 * FF + 3 * D, 2 * FF + 4 * D
FF_TILE = 512
CHUNKS = 4


def dot_nn(a, b):
    return lax.dot_general(a, b, (((1,), (0,)), ((), ())), preferred_element_type=jnp.float32)


def dot_nt(a, b):
    return lax.dot_general(a, b, (((1,), (1,)), ((), ())), preferred_element_type=jnp.float32)


def dot_tn(a, b):
    return lax.dot_general(a, b, (((0,), (0,)), ((), ())), preferred_element_type=jnp.float32)


def row_mean(values):
    return jnp.mean(values, -1, keepdims=True)


def layer_norm(values):
    centered = values - row_mean(values)
    rstd = lax.rsqrt(row_mean(centered * centered) + EPSILON)
    return centered * rstd, rstd


def norm_back(grad, normed, rstd):
    return rstd * (grad - row_mean(grad) - normed * row_mean(grad * normed))


def col_sum(values):
    return jnp.sum(values, 0, keepdims=True)


def layer_kernel(parts, first, last, *refs):
    live_ref = refs[0]
    ins = refs[1 : 1 + parts]
    (mod_ref, wqkv, wqkv_t, wout, wout_t, wup, wup_t, wdown, wdown_t, bqkv, bout, bup, bdown) = refs[
        1 + parts : 14 + parts
    ]
    rest = refs[14 + parts :]
    if not first:
        acc_in, bias_in = rest[:2]
        rest = rest[2:]
    outs = rest[:parts]
    gmod_ref, acc_out, bias_acc, acc, probs_ref, sem = rest[parts : parts + 6]
    if last:
        acc_low = rest[parts + 6]
    step = pl.program_id(0)
    steps = pl.num_programs(0)

    @pl.when(step == 0)
    def _():
        if first:
            acc[...] = jnp.zeros_like(acc)
            bias_acc[...] = jnp.zeros_like(bias_acc)
        else:
            copy = pltpu.make_async_copy(acc_in, acc, sem)
            copy.start()
            bias_acc[...] = bias_in[...]
            copy.wait()

    rows = ins[0].shape[2]
    full = parts * rows
    tokens = jnp.concatenate([ref[0, 0] for ref in ins], 0).astype(jnp.float32)
    live_parts = [live_ref[step, p] for p in range(parts)]
    live = jnp.concatenate([jnp.full((rows, 1), flag, jnp.float32) for flag in live_parts], 0)
    key_part = lax.broadcasted_iota(jnp.int32, (1, full), 1) // rows
    live_keys = jnp.zeros((1, full), jnp.float32)
    for p in range(parts):
        live_keys = jnp.where(key_part == p, live_parts[p], live_keys)
    live_keys = live_keys > 0.5
    mod = mod_ref[0]
    shift_one, scale_one, gate_one = mod[0:1], 1.0 + mod[1:2], mod[2:3]
    shift_two, scale_two, gate_two = mod[3:4], 1.0 + mod[4:5], mod[5:6]

    norm_one, rstd_one = layer_norm(tokens)
    in_one = (norm_one * scale_one + shift_one).astype(jnp.bfloat16)
    projected = dot_nn(in_one, wqkv[...]) + bqkv[...]
    inv_root = 1.0 / math.sqrt(HEAD_DIM)
    queries = (projected[:, :D].astype(jnp.bfloat16) * jnp.bfloat16(inv_root)).astype(jnp.bfloat16)
    keys = projected[:, D : 2 * D].astype(jnp.bfloat16)
    values = projected[:, 2 * D :].astype(jnp.bfloat16)
    lanes = lax.broadcasted_iota(jnp.int32, (1, 2 * HEAD_DIM), 1)
    halves = (lanes < HEAD_DIM, lanes >= HEAD_DIM)

    def pair(array, j):
        return array[:, j * 2 * HEAD_DIM : (j + 1) * 2 * HEAD_DIM]

    def half(array, h):
        return jnp.where(halves[h], array, jnp.zeros_like(array))

    attended = []
    for j in range(HEADS // 2):
        total = None
        for h in range(2):
            scores = dot_nt(pair(queries, j), half(pair(keys, j), h))
            scores = jnp.where(live_keys, scores, -1e30)
            exps = jnp.exp(scores - jnp.max(scores, -1, keepdims=True))
            probs = exps * (1.0 / jnp.sum(exps, -1, keepdims=True))
            probs_ref[2 * j + h] = probs
            term = dot_nn(probs.astype(jnp.bfloat16), half(pair(values, j), h))
            total = term if total is None else total + term
        attended.append(total.astype(jnp.bfloat16))
    attended = jnp.concatenate(attended, 1)
    attn_branch = dot_nn(attended, wout[...]) + bout[...]
    live_gate_one = live * gate_one
    residual = tokens + live_gate_one * attn_branch
    norm_two, rstd_two = layer_norm(residual)
    in_two = (norm_two * scale_two + shift_two).astype(jnp.bfloat16)

    g_output = jnp.concatenate([ref[1, 0] for ref in ins], 0).astype(jnp.float32)
    live_out = live * g_output
    g_ffn = (live_out * gate_two).astype(jnp.bfloat16)
    in_two_t = in_two.T
    g_ffn_t = g_ffn.T
    ffn = None
    g_in_two = None
    root = math.sqrt(2.0 / math.pi)
    for tile in range(FF // FF_TILE):
        cols = slice(tile * FF_TILE, (tile + 1) * FF_TILE)
        pre = dot_nn(in_two, wup[:, cols]) + bup[:, cols]
        square = pre * pre
        gate = 0.5 + 0.5 * jnp.tanh(pre * (root + (root * 0.044715) * square))
        hidden_wide = pre * gate
        slope = gate + hidden_wide * (1.0 - gate) * (2.0 * root + (6.0 * root * 0.044715) * square)
        hidden = hidden_wide.astype(jnp.bfloat16)
        term = dot_nn(hidden, wdown[cols, :])
        ffn = term if ffn is None else ffn + term
        g_pre_wide = dot_nn(g_ffn, wdown_t[:, cols]) * slope
        g_pre = g_pre_wide.astype(jnp.bfloat16)
        acc[:, DOWN + tile * FF_TILE : DOWN + (tile + 1) * FF_TILE] += dot_nn(g_ffn_t, hidden)
        acc[:, UP + tile * FF_TILE : UP + (tile + 1) * FF_TILE] += dot_nn(in_two_t, g_pre)
        bias_acc[:, UP + tile * FF_TILE : UP + (tile + 1) * FF_TILE] += col_sum(g_pre.astype(jnp.float32))
        term = dot_nn(g_pre, wup_t[cols, :])
        g_in_two = term if g_in_two is None else g_in_two + term
    bias_acc[:, DOWN : DOWN + D] += col_sum(g_ffn.astype(jnp.float32))
    ffn = ffn + bdown[...]
    layer_out = (residual + live * gate_two * ffn).astype(jnp.bfloat16)
    for p in range(parts):
        outs[p][0, 0] = layer_out[p * rows : (p + 1) * rows]
    gmod_ref[0, 5:6] = col_sum(live_out * ffn)
    gmod_ref[0, 4:5] = col_sum(g_in_two * norm_two)
    gmod_ref[0, 3:4] = col_sum(g_in_two)
    g_residual = g_output + norm_back(g_in_two * scale_two, norm_two, rstd_two)
    g_attn = (live_gate_one * g_residual).astype(jnp.bfloat16)
    gmod_ref[0, 2:3] = col_sum(live * g_residual * attn_branch)
    acc[:, OUT : OUT + D] += dot_tn(attended, g_attn)
    bias_acc[:, OUT : OUT + D] += col_sum(g_attn.astype(jnp.float32))
    g_attended = dot_nn(g_attn, wout_t[...]).astype(jnp.bfloat16)

    g_queries, g_keys, g_values = [], [], []
    for j in range(HEADS // 2):
        gq = gk = gv = None
        for h in range(2):
            probs = probs_ref[2 * j + h]
            g_probs = dot_nt(pair(g_attended, j), half(pair(values, j), h))
            weighted = probs * g_probs
            g_scores = (weighted - probs * jnp.sum(weighted, -1, keepdims=True)).astype(jnp.bfloat16)
            tq = dot_nn(g_scores, half(pair(keys, j), h))
            tk = dot_tn(g_scores, half(pair(queries, j), h))
            tv = dot_tn(probs.astype(jnp.bfloat16), half(pair(g_attended, j), h))
            gq, gk, gv = (tq, tk, tv) if gq is None else (gq + tq, gk + tk, gv + tv)
        g_queries.append((gq * inv_root).astype(jnp.bfloat16))
        g_keys.append(gk.astype(jnp.bfloat16))
        g_values.append(gv.astype(jnp.bfloat16))
    g_projected = jnp.concatenate(g_queries + g_keys + g_values, 1)
    acc[:, QKV : QKV + 3 * D] += dot_tn(in_one, g_projected)
    bias_acc[:, QKV : QKV + 3 * D] += col_sum(g_projected.astype(jnp.float32))
    g_in_one = dot_nn(g_projected, wqkv_t[...])
    gmod_ref[0, 1:2] = col_sum(g_in_one * norm_one)
    gmod_ref[0, 0:1] = col_sum(g_in_one)
    g_tokens = (g_residual + norm_back(g_in_one * scale_one, norm_one, rstd_one)).astype(jnp.bfloat16)
    for p in range(parts):
        outs[p][1, 0] = g_tokens[p * rows : (p + 1) * rows]

    @pl.when(step == steps - 1)
    def _():
        if last:
            acc_low[...] = acc[...].astype(jnp.bfloat16)
            copy = pltpu.make_async_copy(acc_low, acc_out, sem)
        else:
            copy = pltpu.make_async_copy(acc, acc_out, sem)
        copy.start()
        copy.wait()


def layer_call(live, blocks, mod, weights, carried, last):
    parts = len(blocks)
    images, rows = blocks[0].shape[1:3]
    first = carried is None
    resident = [pl.BlockSpec(w.shape, lambda i: (0, 0), pipeline_mode=pl.Buffered(1)) for w in weights]
    block_spec = pl.BlockSpec((2, 1, rows, D), lambda i: (0, i, 0, 0))
    mod_spec = pl.BlockSpec((1, 6, D), lambda i: (i, 0, 0))
    any_spec = pl.BlockSpec(memory_space=pl.ANY)
    bias_spec = pl.BlockSpec((1, WIDE), lambda i: (0, 0))
    in_specs = (
        [pl.BlockSpec(memory_space=pltpu.SMEM)] + [block_spec] * parts + [mod_spec] + resident
    )
    args = [live, *blocks, mod, *weights]
    aliases = {}
    if not first:
        in_specs += [any_spec, bias_spec]
        if not last:
            aliases = {len(args): parts + 1}
        args += list(carried)
    acc_type = jnp.bfloat16 if last else jnp.float32
    scratch = [
        pltpu.VMEM((D, WIDE), jnp.float32),
        pltpu.VMEM((HEADS, parts * rows, parts * rows), jnp.float32),
        pltpu.SemaphoreType.DMA,
    ]
    if last:
        scratch.append(pltpu.VMEM((D, WIDE), jnp.bfloat16))
    result = pl.pallas_call(
        functools.partial(layer_kernel, parts, first, last),
        grid=(images,),
        in_specs=in_specs,
        out_specs=[block_spec] * parts + [mod_spec, any_spec, bias_spec],
        out_shape=[jax.ShapeDtypeStruct(b.shape, jnp.bfloat16) for b in blocks]
        + [
            jax.ShapeDtypeStruct((images, 6, D), jnp.float32),
            jax.ShapeDtypeStruct((D, WIDE), acc_type),
            jax.ShapeDtypeStruct((1, WIDE), jnp.float32),
        ],
        scratch_shapes=scratch,
        input_output_aliases=aliases,
        compiler_params=pltpu.CompilerParams(vmem_limit_bytes=52 * 1024 * 1024),
    )(*args)
    return result[:parts], result[parts], (result[parts + 1], result[parts + 2])


def cut(array, start, size, axis=0):
    return lax.dynamic_slice_in_dim(array, start, size, axis)


def group_stages(size):
    bits = [1 << k for k in range(size.bit_length() - 1)]
    if size == 8:
        table = [[1] * 8, [2 if i % 2 == 0 else 4 for i in range(8)], [4 if i % 2 == 0 else 2 for i in range(8)]]
    else:
        table = [[bit] * size for bit in bits]
    return table


def stage_bit(stage, index):
    masks = jnp.asarray(stage, jnp.int32)[index] if len(set(stage)) > 1 else stage[0]
    return jnp.where((index & masks) != 0, 1, 0)


def swap(array, stage):
    return lax.ppermute(array, "grp", [(i, i ^ bit) for i, bit in enumerate(stage)])


def seq_shift(array, shift, size):
    return lax.ppermute(array, "seq", [(i, (i + shift) % size) for i in range(size)])


def reduce_all(array, group, seq):
    index = lax.axis_index("grp")
    place = lax.axis_index("seq")
    stages = group_stages(group)
    for stage in stages:
        size = array.shape[0] // 2
        bit = stage_bit(stage, index)
        got = swap(cut(array, (1 - bit) * size, size), stage)
        array = (cut(array, bit * size, size).astype(jnp.float32) + got.astype(jnp.float32)).astype(jnp.bfloat16)
    size = array.shape[1] // seq
    total = cut(array, place * size, size, 1).astype(jnp.float32)
    for shift in (2, 1, 3) if seq == 4 else range(1, seq):
        total = total + seq_shift(cut(array, ((place + shift) % seq) * size, size, 1), shift, seq).astype(jnp.float32)
    array = gather_seq(total.astype(jnp.bfloat16), place, seq, 1)
    return gather_group(array, index, stages)


def gather_seq(array, place, seq, axis):
    size = array.shape[axis]
    shape = list(array.shape)
    shape[axis] = size * seq
    whole = lax.dynamic_update_slice_in_dim(jnp.zeros(shape, array.dtype), array, place * size, axis)
    for shift in (2, 1, 3) if seq == 4 else range(1, seq):
        got = seq_shift(array, shift, seq)
        whole = lax.dynamic_update_slice_in_dim(whole, got, ((place - shift) % seq) * size, axis)
    return whole


def gather_group(array, index, stages):
    for stage in reversed(stages):
        bit = stage_bit(stage, index)
        got = swap(array, stage)
        array = jnp.where(bit == 0, jnp.concatenate([array, got], 0), jnp.concatenate([got, array], 0))
    return array


def shards(
    group,
    seq,
    tokens,
    cotangent,
    condition,
    mask_flags,
    noise_levels,
    level_table,
    ada_weight,
    ada_bias,
    qkv_weight,
    query_value_bias,
    output_weight,
    output_bias,
    up_weight,
    up_bias,
    down_weight,
    down_bias,
):
    batches, images, rows = tokens.shape[:3]
    count = batches * images
    own = count // seq
    step = own // CHUNKS
    place = lax.axis_index("seq")
    index = lax.axis_index("grp")
    stages = group_stages(group)
    tokens = tokens.reshape(count, rows, D)
    cotangent = cotangent.reshape(count, rows, D)
    shifts = (0, 2, 1, 3) if seq == 4 else tuple(range(seq))

    def fetch(chunk):
        blocks = []
        for shift in shifts:
            start = ((place + shift) % seq) * own + chunk * step
            block = jnp.stack([cut(tokens, start, step), cut(cotangent, start, step)])
            blocks.append(block if shift == 0 else seq_shift(block, shift, seq))
        return blocks

    flags = cut(mask_flags.reshape(count), place * own, own)
    sources = jnp.stack([(place - shift) % seq for shift in shifts])
    kept = sources * rows < KEEP
    live = jnp.logical_or(flags[:, None] == 0, kept[None, :]).astype(jnp.float32)

    table = jnp.concatenate(
        [condition.reshape(count, D), jnp.broadcast_to(noise_levels.reshape(count, 1).astype(jnp.float32), (count, 128))],
        1,
    )
    gathered = gather_group_plain(table, index, group)
    onehot = (gathered[:, D : D + 1].astype(jnp.int32) == jnp.arange(LEVELS, dtype=jnp.int32)[None, :]).astype(
        jnp.float32
    )
    cond_full = gathered[:, :D] + jnp.dot(onehot, level_table, precision=highest)
    activated = jax.nn.silu(cond_full).astype(jnp.bfloat16)
    mine = (noise_levels.reshape(count)[:, None] == jnp.arange(LEVELS, dtype=jnp.int32)[None, :]).astype(jnp.float32)
    mine = cut(condition.reshape(count, D), place * own, own) + jnp.dot(
        cut(mine, place * own, own), level_table, precision=highest
    )
    modulation = (
        jnp.dot(jax.nn.silu(mine).astype(jnp.bfloat16), ada_weight, preferred_element_type=jnp.float32) + ada_bias
    ).reshape(own, 6, D)

    bias_full = jnp.concatenate([query_value_bias[:D], jnp.zeros((D,), jnp.float32), query_value_bias[D:]])
    weights = (
        qkv_weight,
        qkv_weight.T,
        output_weight,
        output_weight.T,
        up_weight,
        up_weight.T,
        down_weight,
        down_weight.T,
        bias_full[None],
        output_bias[None],
        up_bias[None],
        down_bias[None],
    )
    out_rows = jnp.zeros((count, rows, D), jnp.bfloat16)
    grad_rows = jnp.zeros((count, rows, D), jnp.bfloat16)
    carried = None
    g_mods = []
    blocks = fetch(0)
    for chunk in range(CHUNKS):
        following = fetch(chunk + 1) if chunk + 1 < CHUNKS else None
        span = slice(chunk * step, (chunk + 1) * step)
        results, g_mod, carried = layer_call(
            live[span], blocks, modulation[span], weights, carried, chunk + 1 == CHUNKS
        )
        g_mods.append(g_mod)
        for shift, result in zip(shifts, results):
            back = result if shift == 0 else seq_shift(result, -shift, seq)
            start = ((place + shift) % seq) * own + chunk * step
            out_rows = lax.dynamic_update_slice_in_dim(out_rows, back[0], start, 0)
            grad_rows = lax.dynamic_update_slice_in_dim(grad_rows, back[1], start, 0)
        blocks = following

    summed, bias_sums = carried
    flat = jnp.concatenate([jnp.concatenate(g_mods).reshape(-1), bias_sums.reshape(-1)])
    lines = -(-flat.shape[0] // 2048) * 16
    flat = jnp.pad(flat, (0, lines * 128 - flat.shape[0])).reshape(lines, 128).astype(jnp.bfloat16)
    small = gather_seq(flat, place, seq, 0)
    small = gather_group_plain(small, index, group).reshape(group * seq, lines * 128)
    g_all = small[:, : own * 6 * D].reshape(group * count, 6 * D)
    bias_all = jnp.sum(small[:, own * 6 * D : own * 6 * D + WIDE].astype(jnp.float32), 0)

    grad_ada = lax.dot_general(activated, g_all, (((0,), (0,)), ((), ())), preferred_element_type=jnp.float32)
    grad_ada_bias = jnp.sum(g_all.astype(jnp.float32), 0)
    g_activated = lax.dot_general(g_all, ada_weight, (((1,), (1,)), ((), ())), preferred_element_type=jnp.float32)
    g_cond = jax.vjp(jax.nn.silu, cond_full)[1](g_activated)[0]
    grad_level = lax.dot_general(
        onehot, g_cond, (((0,), (0,)), ((), ())), precision=highest, preferred_element_type=jnp.float32
    )
    grad_condition = cut(g_cond, index * count, count).reshape(batches, images, D)

    summed = reduce_all(summed, group, seq)
    grad_down = summed[:, DOWN : DOWN + FF].T.astype(jnp.float32)
    return (
        out_rows.reshape(batches, images, rows, D),
        grad_rows.reshape(batches, images, rows, D),
        grad_condition,
        grad_level,
        grad_ada,
        grad_ada_bias,
        summed[:, QKV : QKV + 3 * D].astype(jnp.float32),
        jnp.concatenate([bias_all[QKV : QKV + D], bias_all[QKV + 2 * D : QKV + 3 * D]]),
        summed[:, OUT : OUT + D].astype(jnp.float32),
        bias_all[OUT : OUT + D],
        summed[:, UP : UP + FF].astype(jnp.float32),
        bias_all[UP : UP + FF],
        grad_down,
        bias_all[DOWN : DOWN + D],
    )


def gather_group_plain(array, index, group):
    size = array.shape[0]
    bit = 1
    while bit < group:
        got = swap(array, [bit] * group)
        high = (index & bit) != 0
        array = jnp.where(high, jnp.concatenate([got, array], 0), jnp.concatenate([array, got], 0))
        bit *= 2
    return array.reshape((group * size,) + array.shape[1:])


def solution(mesh):
    rows = P(None, "grp", "seq", None)
    in_specs = (rows, rows, P(None, "grp", None), P(None, "grp"), P(None, "grp")) + (P(),) * 11
    out_specs = (rows, rows, P(None, "grp", None)) + (P(),) * 11
    body = functools.partial(shards, mesh.shape["grp"], mesh.shape["seq"])
    return jax.shard_map(body, mesh=mesh, in_specs=in_specs, out_specs=out_specs, check_vma=False)
```

```python
import functools
import math

import jax
import jax.numpy as jnp
from jax import lax
from jax.experimental import pallas as pl
from jax.experimental.pallas import tpu as pltpu
from jax.sharding import PartitionSpec as P

D = 384
HEADS = 6
HEAD_DIM = 64
FF = 1536
SEQ_LEN = 256
KEEP = 128
LEVELS = 64
EPSILON = 1e-06
highest = lax.Precision.HIGHEST

UP, DOWN, QKV, OUT, WIDE = 0, FF, 2 * FF, 2 * FF + 3 * D, 2 * FF + 4 * D
FF_TILE = 1536
CHUNKS = (2, 3, 3)
GROUPS = ((0, 1), (2,))
PAD = 8
KERNEL_FLOPS = 30_000_000_000


def dot_nn(a, b):
    return lax.dot_general(a, b, (((1,), (0,)), ((), ())), preferred_element_type=jnp.float32)


def dot_nt(a, b):
    return lax.dot_general(a, b, (((1,), (1,)), ((), ())), preferred_element_type=jnp.float32)


def dot_tn(a, b):
    return lax.dot_general(a, b, (((0,), (0,)), ((), ())), preferred_element_type=jnp.float32)


def row_mean(values):
    return jnp.mean(values, -1, keepdims=True)


def layer_norm(values):
    centered = values - row_mean(values)
    rstd = lax.rsqrt(row_mean(centered * centered) + EPSILON)
    return centered * rstd, rstd


def norm_back(grad, normed, rstd):
    return rstd * (grad - row_mean(grad) - normed * row_mean(grad * normed))


def col_sum(values):
    return jnp.sum(values, 0, keepdims=True)


def layer_kernel(parts, first, last, placed, *refs):
    live_ref = refs[0]
    ins = refs[1 : 1 + parts]
    (mod_ref, wqkv, wout, wup, wdown, bqkv, bout, bup, bdown) = refs[1 + parts : 10 + parts]
    rest = refs[10 + parts :]
    if not first:
        acc_in, bias_in = rest[:2]
        rest = rest[2:]
    if placed:
        rest = rest[parts:]
    outs = rest[:parts]
    gmod_ref, acc_out, bias_acc, acc, probs_ref, sem = rest[parts : parts + 6]
    acc_low = rest[parts + 6] if last else acc
    step = pl.program_id(0)
    steps = pl.num_programs(0)

    def send(start, stop, slot):
        @pl.when(step == steps - 1)
        def _():
            if last:
                acc_low[:, start:stop] = acc[:, start:stop].astype(jnp.bfloat16)
            sent(start, stop, slot).start()

    def sent(start, stop, slot):
        return pltpu.make_async_copy(acc_low.at[:, start:stop], acc_out.at[:, start:stop], sem.at[slot])

    @pl.when(step == 0)
    def _():
        if first:
            acc[...] = jnp.zeros_like(acc)
            bias_acc[...] = jnp.zeros_like(bias_acc)
        else:
            pltpu.make_async_copy(acc_in, acc, sem.at[0]).start()
            bias_acc[...] = bias_in[...]

    rows = ins[0].shape[2]
    full = parts * rows
    tokens = jnp.concatenate([ref[0, 0] for ref in ins], 0).astype(jnp.float32)
    live_parts = [live_ref[step, p] for p in range(parts)]
    live = jnp.concatenate([jnp.full((rows, 1), flag, jnp.float32) for flag in live_parts], 0)
    key_part = lax.broadcasted_iota(jnp.int32, (1, full), 1) // rows
    live_keys = jnp.zeros((1, full), jnp.float32)
    for p in range(parts):
        live_keys = jnp.where(key_part == p, live_parts[p], live_keys)
    live_keys = live_keys > 0.5
    mod = mod_ref[0]
    shift_one, scale_one, gate_one = mod[0:1], 1.0 + mod[1:2], mod[2:3]
    shift_two, scale_two, gate_two = mod[3:4], 1.0 + mod[4:5], mod[5:6]

    norm_one, rstd_one = layer_norm(tokens)
    in_one = (norm_one * scale_one + shift_one).astype(jnp.bfloat16)
    projected = dot_nn(in_one, wqkv[...]) + bqkv[...]
    inv_root = 1.0 / math.sqrt(HEAD_DIM)
    queries = (projected[:, :D].astype(jnp.bfloat16) * jnp.bfloat16(inv_root)).astype(jnp.bfloat16)
    keys = projected[:, D : 2 * D].astype(jnp.bfloat16)
    values = projected[:, 2 * D :].astype(jnp.bfloat16)
    lanes = lax.broadcasted_iota(jnp.int32, (1, 2 * HEAD_DIM), 1)
    halves = (lanes < HEAD_DIM, lanes >= HEAD_DIM)

    def pair(array, j):
        return array[:, j * 2 * HEAD_DIM : (j + 1) * 2 * HEAD_DIM]

    def half(array, h):
        return jnp.where(halves[h], array, jnp.zeros_like(array))

    def head_scores(n):
        j, h = divmod(n, 2)
        return jnp.where(live_keys, dot_nt(pair(queries, j), half(pair(keys, j), h)), -1e30)

    attended = []
    every = [head_scores(n) for n in range(HEADS)]
    for n in range(HEADS):
        scores, ahead = every[n], None
        j, h = divmod(n, 2)
        exps = jnp.exp(scores - jnp.max(scores, -1, keepdims=True))
        probs = exps * (1.0 / jnp.sum(exps, -1, keepdims=True))
        probs_ref[n] = probs
        term = dot_nn(probs.astype(jnp.bfloat16), half(pair(values, j), h))
        if h == 0:
            total = term
        else:
            attended.append((total + term).astype(jnp.bfloat16))
        scores = ahead
    attended = jnp.concatenate(attended, 1)
    attn_branch = dot_nn(attended, wout[...]) + bout[...]
    live_gate_one = live * gate_one
    residual = tokens + live_gate_one * attn_branch
    norm_two, rstd_two = layer_norm(residual)
    in_two = (norm_two * scale_two + shift_two).astype(jnp.bfloat16)

    g_output = jnp.concatenate([ref[1, 0] for ref in ins], 0).astype(jnp.float32)
    live_out = live * g_output
    g_ffn = (live_out * gate_two).astype(jnp.bfloat16)
    if not first:

        @pl.when(step == 0)
        def _():
            pltpu.make_async_copy(acc_in, acc, sem.at[0]).wait()

    in_two_t = in_two.T
    g_ffn_t = g_ffn.T
    ffn = None
    g_in_two = None
    root = math.sqrt(2.0 / math.pi)
    for tile in range(FF // FF_TILE):
        cols = slice(tile * FF_TILE, (tile + 1) * FF_TILE)
        pre = dot_nn(in_two, wup[:, cols]) + bup[:, cols]
        square = pre * pre
        gate = 0.5 + 0.5 * jnp.tanh(pre * (root + (root * 0.044715) * square))
        hidden_wide = pre * gate
        slope = gate + hidden_wide * (1.0 - gate) * (2.0 * root + (6.0 * root * 0.044715) * square)
        hidden = hidden_wide.astype(jnp.bfloat16)
        term = dot_nn(hidden, wdown[cols, :])
        ffn = term if ffn is None else ffn + term
        g_pre_wide = dot_nt(g_ffn, wdown[cols, :]) * slope
        g_pre = g_pre_wide.astype(jnp.bfloat16)
        acc[:, DOWN + tile * FF_TILE : DOWN + (tile + 1) * FF_TILE] += dot_nn(g_ffn_t, hidden)
        acc[:, UP + tile * FF_TILE : UP + (tile + 1) * FF_TILE] += dot_nn(in_two_t, g_pre)
        bias_acc[:, UP + tile * FF_TILE : UP + (tile + 1) * FF_TILE] += col_sum(g_pre.astype(jnp.float32))
        term = dot_nt(g_pre, wup[:, cols])
        g_in_two = term if g_in_two is None else g_in_two + term
    send(UP, QKV, 0)
    bias_acc[:, DOWN : DOWN + D] += col_sum(g_ffn.astype(jnp.float32))
    ffn = ffn + bdown[...]
    layer_out = (residual + live * gate_two * ffn).astype(jnp.bfloat16)
    for p in range(parts):
        outs[p][0, 0] = layer_out[p * rows : (p + 1) * rows]
    gmod_ref[0, 5:6] = col_sum(live_out * ffn)
    gmod_ref[0, 4:5] = col_sum(g_in_two * norm_two)
    gmod_ref[0, 3:4] = col_sum(g_in_two)
    g_residual = g_output + norm_back(g_in_two * scale_two, norm_two, rstd_two)
    g_attn = (live_gate_one * g_residual).astype(jnp.bfloat16)
    gmod_ref[0, 2:3] = col_sum(live * g_residual * attn_branch)
    acc[:, OUT : OUT + D] += dot_tn(attended, g_attn)
    bias_acc[:, OUT : OUT + D] += col_sum(g_attn.astype(jnp.float32))
    g_attended = dot_nt(g_attn, wout[...]).astype(jnp.bfloat16)

    g_queries, g_keys, g_values = [], [], []

    def head_probs(n):
        j, h = divmod(n, 2)
        return dot_nt(pair(g_attended, j), half(pair(values, j), h))

    queries_t = queries.T
    g_attended_t = g_attended.T
    every = [head_probs(n) for n in range(HEADS)]
    for n in range(HEADS):
        j, h = divmod(n, 2)
        head = slice(n * HEAD_DIM, (n + 1) * HEAD_DIM)
        probs = probs_ref[n]
        weighted = probs * every[n]
        g_scores = (weighted - probs * jnp.sum(weighted, -1, keepdims=True)).astype(jnp.bfloat16)
        tq = dot_nn(g_scores, half(pair(keys, j), h))
        g_keys.append(dot_nn(queries_t[head], g_scores).astype(jnp.bfloat16))
        g_values.append(dot_nn(g_attended_t[head], probs.astype(jnp.bfloat16)).astype(jnp.bfloat16))
        if h == 0:
            gq = tq
        else:
            g_queries.append(((gq + tq) * inv_root).astype(jnp.bfloat16))
    g_keys = [jnp.concatenate(g_keys, 0).T]
    g_values = [jnp.concatenate(g_values, 0).T]
    g_projected = jnp.concatenate(g_queries + g_keys + g_values, 1)
    acc[:, QKV : QKV + 3 * D] += dot_tn(in_one, g_projected)
    send(QKV, WIDE, 1)
    bias_acc[:, QKV : QKV + 3 * D] += col_sum(g_projected.astype(jnp.float32))
    g_in_one = dot_nt(g_projected, wqkv[...])
    gmod_ref[0, 1:2] = col_sum(g_in_one * norm_one)
    gmod_ref[0, 0:1] = col_sum(g_in_one)
    g_tokens = (g_residual + norm_back(g_in_one * scale_one, norm_one, rstd_one)).astype(jnp.bfloat16)
    for p in range(parts):
        outs[p][1, 0] = g_tokens[p * rows : (p + 1) * rows]

    @pl.when(step == steps - 1)
    def _():
        sent(UP, QKV, 0).wait()
        sent(QKV, WIDE, 1).wait()


def layer_call(live, blocks, mod, weights, carried, buffers, place, size, last):
    parts = len(blocks)
    images, rows = blocks[0].shape[1:3]
    first = carried is None
    resident = [pl.BlockSpec(w.shape, lambda i: (0, 0), pipeline_mode=pl.Buffered(1)) for w in weights]
    block_spec = pl.BlockSpec((2, 1, rows, D), lambda i: (0, i, 0, 0))
    out_spec = pl.BlockSpec((2, 1, rows, D), lambda i: (0, i + place, 0, 0))
    mod_spec = pl.BlockSpec((1, 6, D), lambda i: (i, 0, 0))
    any_spec = pl.BlockSpec(memory_space=pl.ANY)
    bias_spec = pl.BlockSpec((1, WIDE), lambda i: (0, 0))
    in_specs = (
        [pl.BlockSpec(memory_space=pltpu.SMEM)] + [block_spec] * parts + [mod_spec] + resident
    )
    args = [live, *blocks, mod, *weights]
    aliases = {}
    if not first:
        in_specs += [any_spec, bias_spec]
        if not last:
            aliases[len(args)] = parts + 1
        args += list(carried)
    if buffers is not None:
        in_specs += [any_spec] * parts
        aliases.update({len(args) + p: p for p in range(parts)})
        args += list(buffers)
    acc_type = jnp.bfloat16 if last else jnp.float32
    scratch = [
        pltpu.VMEM((D, WIDE), jnp.float32),
        pltpu.VMEM((HEADS, parts * rows, parts * rows), jnp.float32),
        pltpu.SemaphoreType.DMA((2,)),
    ]
    if last:
        scratch.append(pltpu.VMEM((D, WIDE), jnp.bfloat16))
    result = pl.pallas_call(
        functools.partial(layer_kernel, parts, first, last, buffers is not None),
        grid=(images,),
        in_specs=in_specs,
        out_specs=[out_spec] * parts + [mod_spec, any_spec, bias_spec],
        out_shape=[jax.ShapeDtypeStruct((2, size, rows, D), jnp.bfloat16)] * parts
        + [
            jax.ShapeDtypeStruct((images, 6, D), jnp.float32),
            jax.ShapeDtypeStruct((D, WIDE), acc_type),
            jax.ShapeDtypeStruct((1, WIDE), jnp.float32),
        ],
        scratch_shapes=scratch,
        input_output_aliases=aliases,
        cost_estimate=pl.CostEstimate(
            flops=KERNEL_FLOPS * images, transcendentals=0, bytes_accessed=8 * images * parts * rows * D
        ),
        compiler_params=pltpu.CompilerParams(vmem_limit_bytes=52 * 1024 * 1024),
    )(*args)
    return result[:parts], result[parts], (result[parts + 1], result[parts + 2])


def finish_kernel(bit_ref, mine_ref, other_ref, up_ref, down_ref, qkv_ref, out_ref):
    low = bit_ref[0] == 0
    size = mine_ref.shape[0]
    mine, other = mine_ref[...], other_ref[...]
    down = []
    for k in range(2):
        part = jnp.where(low, mine, other) if k == 0 else jnp.where(low, other, mine)
        span = slice(k * size, (k + 1) * size)
        up_ref[span] = part[:, UP : UP + FF].astype(jnp.float32)
        qkv_ref[span] = part[:, QKV : QKV + 3 * D].astype(jnp.float32)
        out_ref[span] = part[:, OUT : OUT + D].astype(jnp.float32)
        down.append(part[:, DOWN : DOWN + FF])
    down_ref[...] = jnp.concatenate(down, 0).T.astype(jnp.float32)


def finish(bit, mine, other):
    full = pl.BlockSpec(memory_space=pltpu.VMEM)
    rows = 2 * mine.shape[0]
    shapes = [(rows, FF), (FF, rows), (rows, 3 * D), (rows, D)]
    return pl.pallas_call(
        finish_kernel,
        in_specs=[pl.BlockSpec(memory_space=pltpu.SMEM), full, full],
        out_specs=[full] * 4,
        out_shape=[jax.ShapeDtypeStruct(shape, jnp.float32) for shape in shapes],
        compiler_params=pltpu.CompilerParams(vmem_limit_bytes=52 * 1024 * 1024),
    )(bit.reshape(1), mine, other)


def cut(array, start, size, axis=0):
    return lax.dynamic_slice_in_dim(array, start, size, axis)


def group_stages(size):
    bits = [1 << k for k in range(size.bit_length() - 1)]
    if size == 8:
        table = [[1] * 8, [2 if i % 2 == 0 else 4 for i in range(8)], [4 if i % 2 == 0 else 2 for i in range(8)]]
    else:
        table = [[bit] * size for bit in bits]
    return table


def stage_bit(stage, index):
    masks = jnp.asarray(stage, jnp.int32)[index] if len(set(stage)) > 1 else stage[0]
    return jnp.where((index & masks) != 0, 1, 0)


def swap(array, stage):
    return lax.ppermute(array, "grp", [(i, i ^ bit) for i, bit in enumerate(stage)])


def seq_shift(array, shift, size):
    return lax.ppermute(array, "seq", [(i, (i + shift) % size) for i in range(size)])


def scatter_sum(array, index, place, stages, seq):
    for stage in stages:
        size = array.shape[0] // 2
        bit = stage_bit(stage, index)
        got = swap(cut(array, (1 - bit) * size, size), stage)
        array = (cut(array, bit * size, size).astype(jnp.float32) + got.astype(jnp.float32)).astype(jnp.bfloat16)
    size = array.shape[1] // seq
    total = cut(array, place * size, size, 1).astype(jnp.float32)
    for shift in seq_shifts(seq)[1:]:
        total = total + seq_shift(cut(array, ((place + shift) % seq) * size, size, 1), shift, seq).astype(jnp.float32)
    return total.astype(jnp.bfloat16)


def gather_seq(array, place, seq, axis):
    size = array.shape[axis]
    shape = list(array.shape)
    shape[axis] = size * seq
    whole = lax.dynamic_update_slice_in_dim(jnp.zeros(shape, array.dtype), array, place * size, axis)
    for shift in seq_shifts(seq)[1:]:
        got = seq_shift(array, shift, seq)
        whole = lax.dynamic_update_slice_in_dim(whole, got, ((place - shift) % seq) * size, axis)
    return whole


def join(array, index, stage):
    got = swap(array, stage)
    low = stage_bit(stage, index) == 0
    return jnp.where(low, jnp.concatenate([array, got], 0), jnp.concatenate([got, array], 0))


def gather_group(array, index, group):
    bit = 1
    while bit < group:
        array = join(array, index, [bit] * group)
        bit *= 2
    return array


def seq_shifts(seq):
    return (0, 2, 1, 3) if seq == 4 else tuple(range(seq))


def tied(values, after):
    return lax.optimization_barrier((values, after))[0]


def level_rows(levels):
    return (levels[:, None] == jnp.arange(LEVELS, dtype=levels.dtype)[None, :]).astype(jnp.float32)


def shards(
    group,
    seq,
    tokens,
    cotangent,
    condition,
    mask_flags,
    noise_levels,
    level_table,
    ada_weight,
    ada_bias,
    qkv_weight,
    query_value_bias,
    output_weight,
    output_bias,
    up_weight,
    up_bias,
    down_weight,
    down_bias,
):
    batches, images, rows = tokens.shape[:3]
    count = batches * images
    own = count // seq
    place = lax.axis_index("seq")
    index = lax.axis_index("grp")
    stages = group_stages(group)
    shifts = seq_shifts(seq)
    chunks, groups = (CHUNKS, GROUPS) if sum(CHUNKS) == own else ((own,), ((0,),))
    starts = [sum(chunks[:c]) for c in range(len(chunks))]
    whole = (tokens.reshape(count, rows, D), cotangent.reshape(count, rows, D))
    condition = condition.reshape(count, D)
    noise_levels = noise_levels.reshape(count)

    def fetch(chunk, after):
        source = whole if after is None else tied(whole, after)
        blocks = []
        for shift in shifts:
            start = ((place + shift) % seq) * own + starts[chunk]
            block = jnp.stack([cut(array, start, chunks[chunk]) for array in source])
            blocks.append(block if shift == 0 else seq_shift(block, shift, seq))
        return blocks

    blocks = fetch(0, None)

    flags = cut(mask_flags.reshape(count), place * own, own)
    sources = jnp.stack([(place - shift) % seq for shift in shifts])
    live = jnp.logical_or(flags[:, None] == 0, sources[None, :] * rows < KEEP).astype(jnp.float32)

    mine = cut(condition, place * own, own) + jnp.dot(
        level_rows(cut(noise_levels, place * own, own)), level_table, precision=highest
    )
    modulation = (
        jnp.dot(jax.nn.silu(mine).astype(jnp.bfloat16), ada_weight, preferred_element_type=jnp.float32) + ada_bias
    ).reshape(own, 6, D)

    bias_full = jnp.concatenate([query_value_bias[:D], jnp.zeros((D,), jnp.float32), query_value_bias[D:]])
    weights = (
        qkv_weight,
        output_weight,
        up_weight,
        down_weight,
        bias_full[None],
        output_bias[None],
        up_bias[None],
        down_bias[None],
    )
    table = jnp.concatenate(
        [condition, jnp.broadcast_to(noise_levels[:, None].astype(jnp.float32), (count, 128))], 1
    )
    table = gather_group(table, index, group).reshape(group * seq, own, D + 128)
    table = jnp.pad(table, ((0, 0), (0, PAD), (0, 0)), constant_values=-1.0).reshape(-1, D + 128)
    real = table[:, D : D + 1] >= 0.0
    onehot = level_rows(table[:, D].astype(jnp.int32))
    cond_full = jnp.where(real, table[:, :D] + jnp.dot(onehot, level_table, precision=highest), 0.0)
    activated = jax.nn.silu(cond_full).astype(jnp.bfloat16)
    slot = jnp.arange(own + PAD, dtype=jnp.int32)
    picks = jnp.stack([slot < own] + [slot == own + k for k in range(2)] + [slot < 0] * 5)
    picks = jnp.tile(picks.astype(jnp.bfloat16), (1, group * seq))
    live = tied(live, table)

    carried = None
    g_mods = []
    held = []
    for members in groups:
        buffers = None
        total = sum(chunks[c] for c in members)
        for chunk in members:
            following = fetch(chunk + 1, blocks) if chunk + 1 < len(chunks) else None
            span = slice(starts[chunk], starts[chunk] + chunks[chunk])
            buffers, g_mod, carried = layer_call(
                live[span],
                blocks,
                modulation[span],
                weights,
                carried,
                buffers,
                starts[chunk] - starts[members[0]],
                total,
                chunk + 1 == len(chunks),
            )
            g_mods.append(g_mod)
            arrived = blocks
            blocks = following
        held.append(buffers)

    out_rows = jnp.zeros((count, rows, D), jnp.bfloat16)
    grad_rows = jnp.zeros((count, rows, D), jnp.bfloat16)

    def give(targets, members, buffers, after):
        for shift, buffer in zip(shifts, buffers):
            if shift != 0:
                after = back = seq_shift(tied(buffer, after), -shift, seq)
            else:
                back = buffer
            start = ((place + shift) % seq) * own + starts[members[0]]
            targets = [lax.dynamic_update_slice_in_dim(t, back[k], start, 0) for k, t in enumerate(targets)]
        return targets, after

    summed, bias_sums = carried
    small = jnp.concatenate(
        [g.reshape(-1, 6 * D) for g in g_mods]
        + [bias_sums.reshape(2, 6 * D), jnp.zeros((PAD - 2, 6 * D), jnp.float32)]
    ).astype(jnp.bfloat16)
    small = gather_seq(small, place, seq, 0)
    small = gather_group(small, index, group)
    sums = dot_nn(picks, small)
    grad_ada_bias = sums[0]
    bias_all = sums[1:3].reshape(WIDE)
    grad_ada = dot_tn(activated, small)
    g_activated = dot_nt(small, ada_weight)
    g_cond = jax.vjp(jax.nn.silu, cond_full)[1](g_activated)[0]
    grad_level = lax.dot_general(
        onehot, g_cond, (((0,), (0,)), ((), ())), precision=highest, preferred_element_type=jnp.float32
    )
    grad_condition = cut(g_cond, index * seq * (own + PAD), seq * (own + PAD)).reshape(seq, own + PAD, D)[:, :own]

    part = scatter_sum(summed, index, place, stages, seq)
    targets, after = give([out_rows, grad_rows], groups[0], held[0], arrived)
    part = gather_seq(part, place, seq, 1)
    if len(groups) > 1:
        targets, after = give(targets, groups[1], held[1], after)
    for stage in reversed(stages[1:]):
        part = join(part, index, stage)
    grad_up, grad_down, grad_qkv, grad_out = finish(
        stage_bit(stages[0], index), part, swap(part, stages[0])
    )
    return (
        targets[0].reshape(batches, images, rows, D),
        targets[1].reshape(batches, images, rows, D),
        grad_condition.reshape(batches, images, D),
        grad_level,
        grad_ada,
        grad_ada_bias,
        grad_qkv,
        jnp.concatenate([bias_all[QKV : QKV + D], bias_all[QKV + 2 * D : QKV + 3 * D]]),
        grad_out,
        bias_all[OUT : OUT + D],
        grad_up,
        bias_all[UP : UP + FF],
        grad_down,
        bias_all[DOWN : DOWN + D],
    )


def solution(mesh):
    rows = P(None, "grp", "seq", None)
    in_specs = (rows, rows, P(None, "grp", None), P(None, "grp"), P(None, "grp")) + (P(),) * 11
    out_specs = (rows, rows, P(None, "grp", None)) + (P(),) * 11
    body = functools.partial(shards, mesh.shape["grp"], mesh.shape["seq"])
    return jax.shard_map(body, mesh=mesh, in_specs=in_specs, out_specs=out_specs, check_vma=False)
```

```python
import functools
import math

import jax
import jax.numpy as jnp
from jax import lax
from jax.experimental import pallas as pl
from jax.experimental.pallas import tpu as pltpu
from jax.sharding import PartitionSpec as P

D = 384
HEADS = 6
HEAD_DIM = 64
FF = 1536
SEQ_LEN = 256
KEEP = 128
LEVELS = 64
EPSILON = 1e-06
highest = lax.Precision.HIGHEST

UP, DOWN, QKV, OUT, WIDE = 0, FF, 2 * FF, 2 * FF + 3 * D, 2 * FF + 4 * D
FF_TILE = 1536
CHUNKS = (2, 3, 3)
SIDE = 640
COND = 6 * D + SIDE
LEVEL = COND + 2 * D
KERNEL_FLOPS = 30_000_000_000


def dot_nn(a, b):
    return lax.dot_general(a, b, (((1,), (0,)), ((), ())), preferred_element_type=jnp.float32)


def dot_nt(a, b):
    return lax.dot_general(a, b, (((1,), (1,)), ((), ())), preferred_element_type=jnp.float32)


def dot_tn(a, b):
    return lax.dot_general(a, b, (((0,), (0,)), ((), ())), preferred_element_type=jnp.float32)


def row_mean(values):
    return jnp.mean(values, -1, keepdims=True)


def layer_norm(values):
    centered = values - row_mean(values)
    rstd = lax.rsqrt(row_mean(centered * centered) + EPSILON)
    return centered * rstd, rstd


def norm_back(grad, normed, rstd):
    return rstd * (grad - row_mean(grad) - normed * row_mean(grad * normed))


def col_sum(values):
    return jnp.sum(values, 0, keepdims=True)


def layer_kernel(parts, first, last, placed, *refs):
    bit_ref, live_ref = refs[:2]
    refs = refs[1:]
    ins = refs[1 : 1 + parts]
    (mod_ref, wqkv, wout, wup, wdown, bqkv, bout, bup, bdown) = refs[1 + parts : 10 + parts]
    rest = refs[10 + parts :]
    if not first:
        acc_in, bias_in = rest[:2]
        rest = rest[2:]
    if placed:
        rest = rest[parts:]
    outs = rest[:parts]
    gmod_ref, bias_acc, acc_out = rest[parts : parts + 3]
    if last:
        give_out = rest[parts + 3]
        rest = rest[3:]
    acc, probs_ref, sem = rest[parts + 3 : parts + 6]
    acc_low = rest[parts + 6] if last else acc
    step = pl.program_id(0)
    steps = pl.num_programs(0)

    def send(start, stop, slot):
        @pl.when(step == steps - 1)
        def _():
            if last:
                low = bit_ref[0] == 0
                top = acc[: D // 2, start:stop].astype(jnp.bfloat16)
                bottom = acc[D // 2 :, start:stop].astype(jnp.bfloat16)
                acc_low[: D // 2, start:stop] = jnp.where(low, top, bottom)
                acc_low[D // 2 :, start:stop] = jnp.where(low, bottom, top)
            for copy in sent(start, stop, slot):
                copy.start()

    def sent(start, stop, slot):
        if not last:
            return [pltpu.make_async_copy(acc.at[:, start:stop], acc_out.at[:, start:stop], sem.at[slot])]
        return [
            pltpu.make_async_copy(
                acc_low.at[k * (D // 2) : (k + 1) * (D // 2), start:stop], out.at[:, start:stop], sem.at[2 * k + slot]
            )
            for k, out in enumerate((acc_out, give_out))
        ]

    @pl.when(step == 0)
    def _():
        if first:
            acc[...] = jnp.zeros_like(acc)
            bias_acc[...] = jnp.zeros_like(bias_acc)
        else:
            pltpu.make_async_copy(acc_in, acc, sem.at[0]).start()
            bias_acc[...] = bias_in[...]

    rows = ins[0].shape[2]
    full = parts * rows
    tokens = jnp.concatenate([ref[0, 0] for ref in ins], 0).astype(jnp.float32)
    live_parts = [live_ref[step, p] for p in range(parts)]
    live = jnp.concatenate([jnp.full((rows, 1), flag, jnp.float32) for flag in live_parts], 0)
    key_part = lax.broadcasted_iota(jnp.int32, (1, full), 1) // rows
    live_keys = jnp.zeros((1, full), jnp.float32)
    for p in range(parts):
        live_keys = jnp.where(key_part == p, live_parts[p], live_keys)
    live_keys = live_keys > 0.5
    mod = mod_ref[0]
    shift_one, scale_one, gate_one = mod[0:1], 1.0 + mod[1:2], mod[2:3]
    shift_two, scale_two, gate_two = mod[3:4], 1.0 + mod[4:5], mod[5:6]

    norm_one, rstd_one = layer_norm(tokens)
    in_one = (norm_one * scale_one + shift_one).astype(jnp.bfloat16)
    projected = dot_nn(in_one, wqkv[...]) + bqkv[...]
    inv_root = 1.0 / math.sqrt(HEAD_DIM)
    queries = (projected[:, :D].astype(jnp.bfloat16) * jnp.bfloat16(inv_root)).astype(jnp.bfloat16)
    keys = projected[:, D : 2 * D].astype(jnp.bfloat16)
    values = projected[:, 2 * D :].astype(jnp.bfloat16)
    lanes = lax.broadcasted_iota(jnp.int32, (1, 2 * HEAD_DIM), 1)
    halves = (lanes < HEAD_DIM, lanes >= HEAD_DIM)

    def pair(array, j):
        return array[:, j * 2 * HEAD_DIM : (j + 1) * 2 * HEAD_DIM]

    def half(array, h):
        return jnp.where(halves[h], array, jnp.zeros_like(array))

    def head_scores(n):
        j, h = divmod(n, 2)
        return jnp.where(live_keys, dot_nt(pair(queries, j), half(pair(keys, j), h)), -1e30)

    attended = []
    every = [head_scores(n) for n in range(HEADS)]
    for n in range(HEADS):
        scores, ahead = every[n], None
        j, h = divmod(n, 2)
        exps = jnp.exp(scores - jnp.max(scores, -1, keepdims=True))
        probs = exps * (1.0 / jnp.sum(exps, -1, keepdims=True))
        probs_ref[n] = probs
        term = dot_nn(probs.astype(jnp.bfloat16), half(pair(values, j), h))
        if h == 0:
            total = term
        else:
            attended.append((total + term).astype(jnp.bfloat16))
        scores = ahead
    attended = jnp.concatenate(attended, 1)
    attn_branch = dot_nn(attended, wout[...]) + bout[...]
    live_gate_one = live * gate_one
    residual = tokens + live_gate_one * attn_branch
    norm_two, rstd_two = layer_norm(residual)
    in_two = (norm_two * scale_two + shift_two).astype(jnp.bfloat16)

    g_output = jnp.concatenate([ref[1, 0] for ref in ins], 0).astype(jnp.float32)
    live_out = live * g_output
    g_ffn = (live_out * gate_two).astype(jnp.bfloat16)
    if not first:

        @pl.when(step == 0)
        def _():
            pltpu.make_async_copy(acc_in, acc, sem.at[0]).wait()

    in_two_t = in_two.T
    g_ffn_t = g_ffn.T
    ffn = None
    g_in_two = None
    root = math.sqrt(2.0 / math.pi)
    for tile in range(FF // FF_TILE):
        cols = slice(tile * FF_TILE, (tile + 1) * FF_TILE)
        pre = dot_nn(in_two, wup[:, cols]) + bup[:, cols]
        square = pre * pre
        gate = 0.5 + 0.5 * jnp.tanh(pre * (root + (root * 0.044715) * square))
        hidden_wide = pre * gate
        slope = gate + hidden_wide * (1.0 - gate) * (2.0 * root + (6.0 * root * 0.044715) * square)
        hidden = hidden_wide.astype(jnp.bfloat16)
        term = dot_nn(hidden, wdown[cols, :])
        ffn = term if ffn is None else ffn + term
        g_pre_wide = dot_nt(g_ffn, wdown[cols, :]) * slope
        g_pre = g_pre_wide.astype(jnp.bfloat16)
        acc[:, DOWN + tile * FF_TILE : DOWN + (tile + 1) * FF_TILE] += dot_nn(g_ffn_t, hidden)
        acc[:, UP + tile * FF_TILE : UP + (tile + 1) * FF_TILE] += dot_nn(in_two_t, g_pre)
        bias_acc[:, UP + tile * FF_TILE : UP + (tile + 1) * FF_TILE] += col_sum(g_pre.astype(jnp.float32))
        term = dot_nt(g_pre, wup[:, cols])
        g_in_two = term if g_in_two is None else g_in_two + term
    send(UP, QKV, 0)
    bias_acc[:, DOWN : DOWN + D] += col_sum(g_ffn.astype(jnp.float32))
    ffn = ffn + bdown[...]
    layer_out = (residual + live * gate_two * ffn).astype(jnp.bfloat16)
    for p in range(parts):
        outs[p][0, 0] = layer_out[p * rows : (p + 1) * rows]
    gmod_ref[0, 5:6] = col_sum(live_out * ffn)
    gmod_ref[0, 4:5] = col_sum(g_in_two * norm_two)
    gmod_ref[0, 3:4] = col_sum(g_in_two)
    g_residual = g_output + norm_back(g_in_two * scale_two, norm_two, rstd_two)
    g_attn = (live_gate_one * g_residual).astype(jnp.bfloat16)
    gmod_ref[0, 2:3] = col_sum(live * g_residual * attn_branch)
    acc[:, OUT : OUT + D] += dot_tn(attended, g_attn)
    bias_acc[:, OUT : OUT + D] += col_sum(g_attn.astype(jnp.float32))
    g_attended = dot_nt(g_attn, wout[...]).astype(jnp.bfloat16)

    g_queries, g_keys, g_values = [], [], []

    def head_probs(n):
        j, h = divmod(n, 2)
        return dot_nt(pair(g_attended, j), half(pair(values, j), h))

    queries_t = queries.T
    g_attended_t = g_attended.T
    every = [head_probs(n) for n in range(HEADS)]
    for n in range(HEADS):
        j, h = divmod(n, 2)
        head = slice(n * HEAD_DIM, (n + 1) * HEAD_DIM)
        probs = probs_ref[n]
        weighted = probs * every[n]
        g_scores = (weighted - probs * jnp.sum(weighted, -1, keepdims=True)).astype(jnp.bfloat16)
        tq = dot_nn(g_scores, half(pair(keys, j), h))
        g_keys.append(dot_nn(queries_t[head], g_scores).astype(jnp.bfloat16))
        g_values.append(dot_nn(g_attended_t[head], probs.astype(jnp.bfloat16)).astype(jnp.bfloat16))
        if h == 0:
            gq = tq
        else:
            g_queries.append(((gq + tq) * inv_root).astype(jnp.bfloat16))
    g_keys = [jnp.concatenate(g_keys, 0).T]
    g_values = [jnp.concatenate(g_values, 0).T]
    g_projected = jnp.concatenate(g_queries + g_keys + g_values, 1)
    acc[:, QKV : QKV + 3 * D] += dot_tn(in_one, g_projected)
    send(QKV, WIDE, 1)
    bias_acc[:, QKV : QKV + 3 * D] += col_sum(g_projected.astype(jnp.float32))
    g_in_one = dot_nt(g_projected, wqkv[...])
    gmod_ref[0, 1:2] = col_sum(g_in_one * norm_one)
    gmod_ref[0, 0:1] = col_sum(g_in_one)
    g_tokens = (g_residual + norm_back(g_in_one * scale_one, norm_one, rstd_one)).astype(jnp.bfloat16)
    for p in range(parts):
        outs[p][1, 0] = g_tokens[p * rows : (p + 1) * rows]

    @pl.when(step == steps - 1)
    def _():
        for copy in sent(UP, QKV, 0) + sent(QKV, WIDE, 1):
            copy.wait()


def layer_call(bit, live, blocks, mod, weights, carried, buffers, place, size, last, room):
    parts = len(blocks)
    images, rows = blocks[0].shape[1:3]
    first = carried is None
    resident = [pl.BlockSpec(w.shape, lambda i: (0, 0), pipeline_mode=pl.Buffered(1)) for w in weights]
    block_spec = pl.BlockSpec((2, 1, rows, D), lambda i: (0, i, 0, 0))
    out_spec = pl.BlockSpec((2, 1, rows, D), lambda i: (0, i + place, 0, 0))
    mod_spec = pl.BlockSpec((1, 6, D), lambda i: (i, 0, 0))
    any_spec = pl.BlockSpec(memory_space=pl.ANY)
    bias_spec = pl.BlockSpec((1, WIDE), lambda i: (0, 0))
    in_specs = (
        [pl.BlockSpec(memory_space=pltpu.SMEM)] * 2 + [block_spec] * parts + [mod_spec] + resident
    )
    args = [bit.reshape(1), live, *blocks, mod, *weights]
    aliases = {}
    if not first:
        in_specs += [any_spec, bias_spec]
        if not last:
            aliases[len(args)] = parts + 2
        args += list(carried)
    if buffers is not None:
        in_specs += [any_spec] * parts
        aliases.update({len(args) + p: p for p in range(parts)})
        args += list(buffers)
    if last:
        sums = [jax.ShapeDtypeStruct((D // 2, WIDE), jnp.bfloat16)] * 2
        sums += [jax.ShapeDtypeStruct((room, rows, D), jnp.bfloat16)] * 2
    else:
        sums = [jax.ShapeDtypeStruct((D, WIDE), jnp.float32)]
    scratch = [
        pltpu.VMEM((D, WIDE), jnp.float32),
        pltpu.VMEM((HEADS, parts * rows, parts * rows), jnp.float32),
        pltpu.SemaphoreType.DMA((4,)),
    ]
    if last:
        scratch.append(pltpu.VMEM((D, WIDE), jnp.bfloat16))
    result = pl.pallas_call(
        functools.partial(layer_kernel, parts, first, last, buffers is not None),
        grid=(images,),
        in_specs=in_specs,
        out_specs=[out_spec] * parts + [mod_spec, bias_spec] + [any_spec] * len(sums),
        out_shape=[jax.ShapeDtypeStruct((2, size, rows, D), jnp.bfloat16)] * parts
        + [
            jax.ShapeDtypeStruct((images, 6, D), jnp.float32),
            jax.ShapeDtypeStruct((1, WIDE), jnp.float32),
        ]
        + sums,
        scratch_shapes=scratch,
        input_output_aliases=aliases,
        cost_estimate=pl.CostEstimate(
            flops=KERNEL_FLOPS * images, transcendentals=0, bytes_accessed=8 * images * parts * rows * D
        ),
        compiler_params=pltpu.CompilerParams(vmem_limit_bytes=52 * 1024 * 1024),
    )(*args)
    return result[:parts], result[parts], (*result[parts + 2 :], result[parts + 1])


def finish_kernel(bit_ref, mine_ref, other_ref, up_ref, down_ref, qkv_ref, out_ref):
    low = bit_ref[0] == 0
    size = mine_ref.shape[0]
    mine, other = mine_ref[...], other_ref[...]
    down = []
    for k in range(2):
        part = jnp.where(low, mine, other) if k == 0 else jnp.where(low, other, mine)
        span = slice(k * size, (k + 1) * size)
        up_ref[span] = part[:, UP : UP + FF].astype(jnp.float32)
        qkv_ref[span] = part[:, QKV : QKV + 3 * D].astype(jnp.float32)
        out_ref[span] = part[:, OUT : OUT + D].astype(jnp.float32)
        down.append(part[:, DOWN : DOWN + FF])
    down_ref[...] = jnp.concatenate(down, 0).T.astype(jnp.float32)


def finish(bit, mine, other):
    full = pl.BlockSpec(memory_space=pltpu.VMEM)
    rows = 2 * mine.shape[0]
    shapes = [(rows, FF), (FF, rows), (rows, 3 * D), (rows, D)]
    return pl.pallas_call(
        finish_kernel,
        in_specs=[pl.BlockSpec(memory_space=pltpu.SMEM), full, full],
        out_specs=[full] * 4,
        out_shape=[jax.ShapeDtypeStruct(shape, jnp.float32) for shape in shapes],
        compiler_params=pltpu.CompilerParams(vmem_limit_bytes=52 * 1024 * 1024),
    )(bit.reshape(1), mine, other)


def ada_kernel(small_ref, weight_ref, grad_ref, bias_ref, side_ref, cond_out, level_ref):
    rows = small_ref.shape[0]
    small = small_ref[:, : 6 * D]
    slot = lax.broadcasted_iota(jnp.int32, (side_ref.shape[0], rows), 0)
    row = lax.broadcasted_iota(jnp.int32, (side_ref.shape[0], rows), 1)
    picks = (row % side_ref.shape[0] == slot).astype(jnp.bfloat16)
    bias_ref[...] = col_sum(dot_nn(picks, small))
    side_ref[...] = dot_nn(picks, small_ref[:, 6 * D : COND])
    cond = small_ref[:, COND : COND + D].astype(jnp.float32) + small_ref[:, COND + D : LEVEL].astype(jnp.float32)
    gate = jax.nn.sigmoid(cond)
    g_cond = dot_nt(small, weight_ref[...]) * (gate * (1.0 + cond * (1.0 - gate)))
    cond_out[...] = g_cond
    levels = small_ref[:, LEVEL : LEVEL + 128].astype(jnp.float32)
    onehot = (levels == lax.broadcasted_iota(jnp.int32, (rows, 128), 1).astype(jnp.float32)).astype(jnp.float32)
    level_ref[...] = lax.dot_general(
        onehot, g_cond, (((0,), (0,)), ((), ())), precision=highest, preferred_element_type=jnp.float32
    )[:LEVELS]
    grad_ref[...] = dot_tn((cond * gate).astype(jnp.bfloat16), small)


def ada_call(small, weight, own):
    full = pl.BlockSpec(memory_space=pltpu.VMEM)
    rows = small.shape[0]
    shapes = [(D, 6 * D), (1, 6 * D), (own, SIDE), (rows, D), (LEVELS, D)]
    return pl.pallas_call(
        ada_kernel,
        in_specs=[full] * 2,
        out_specs=[full] * 5,
        out_shape=[jax.ShapeDtypeStruct(shape, jnp.float32) for shape in shapes],
        cost_estimate=pl.CostEstimate(flops=6_000_000_000, transcendentals=0, bytes_accessed=8_000_000),
        compiler_params=pltpu.CompilerParams(vmem_limit_bytes=52 * 1024 * 1024),
    )(small, weight)


def cut(array, start, size, axis=0):
    return lax.dynamic_slice_in_dim(array, start, size, axis)


def group_stages(size):
    bits = [1 << k for k in range(size.bit_length() - 1)]
    if size == 8:
        table = [[1] * 8, [2 if i % 2 == 0 else 4 for i in range(8)], [4 if i % 2 == 0 else 2 for i in range(8)]]
    else:
        table = [[bit] * size for bit in bits]
    return table


def stage_bit(stage, index):
    masks = jnp.asarray(stage, jnp.int32)[index] if len(set(stage)) > 1 else stage[0]
    return jnp.where((index & masks) != 0, 1, 0)


def swap(array, stage):
    return lax.ppermute(array, "grp", [(i, i ^ bit) for i, bit in enumerate(stage)])


def seq_shift(array, shift, size):
    return lax.ppermute(array, "seq", [(i, (i + shift) % size) for i in range(size)])


def scatter_grp(keep, give, index, stages, after):
    given = []
    for k, stage in enumerate(stages):
        if k in after:
            give = tied(give, after[k])
        given.append(give)
        got = swap(give, stage)
        if k + 1 < len(stages):
            size = keep.shape[0] // 2
            bit = stage_bit(stages[k + 1], index)
            keep, give = [
                (cut(keep, b * size, size).astype(jnp.float32) + cut(got, b * size, size).astype(jnp.float32)).astype(
                    jnp.bfloat16
                )
                for b in (bit, 1 - bit)
            ]
    return (keep.astype(jnp.float32) + got.astype(jnp.float32)).astype(jnp.bfloat16), given


def scatter_seq(array, place, seq):
    size = array.shape[1] // seq
    total = cut(array, place * size, size, 1).astype(jnp.float32)
    for shift in seq_shifts(seq)[1:]:
        total = total + seq_shift(cut(array, ((place + shift) % seq) * size, size, 1), shift, seq).astype(jnp.float32)
    return total.astype(jnp.bfloat16)


def gather_seq(array, place, seq, axis):
    size = array.shape[axis]
    shape = list(array.shape)
    shape[axis] = size * seq
    whole = lax.dynamic_update_slice_in_dim(jnp.zeros(shape, array.dtype), array, place * size, axis)
    for shift in seq_shifts(seq)[1:]:
        got = seq_shift(array, shift, seq)
        whole = lax.dynamic_update_slice_in_dim(whole, got, ((place - shift) % seq) * size, axis)
    return whole


def join(array, index, stage):
    got = swap(array, stage)
    low = stage_bit(stage, index) == 0
    return jnp.where(low, jnp.concatenate([array, got], 0), jnp.concatenate([got, array], 0))


def join_seq(array, place, bit, seq):
    got = lax.ppermute(array, "seq", [(i, i ^ bit) for i in range(seq)])
    low = (place & bit) == 0
    return jnp.where(low, jnp.concatenate([array, got], 0), jnp.concatenate([got, array], 0))


def join_last(array, index, stage):
    got = swap(array, stage)
    low = stage_bit(stage, index) == 0
    first, second = jnp.where(low, array, got), jnp.where(low, got, array)
    half = first.shape[0] // 2
    odd = (index & 1) == 0
    return jnp.concatenate(
        [
            first[:half],
            jnp.where(odd, second[:half], first[half:]),
            jnp.where(odd, first[half:], second[:half]),
            second[half:],
        ],
        0,
    )


def group_steps(index, group):
    stages = group_stages(group)
    if group == 8:
        stages[1:] = stages[:0:-1]
    steps = [functools.partial(join, index=index, stage=stage) for stage in stages]
    if group == 8:
        steps[-1] = functools.partial(join_last, index=index, stage=stages[-1])
    return steps


def seq_shifts(seq):
    return (0, 2, 1, 3) if seq == 4 else tuple(range(seq))


def tied(values, after):
    return lax.optimization_barrier((values, after))[0]


def level_rows(levels):
    return (levels[:, None] == jnp.arange(LEVELS, dtype=levels.dtype)[None, :]).astype(jnp.float32)


def shards(
    group,
    seq,
    tokens,
    cotangent,
    condition,
    mask_flags,
    noise_levels,
    level_table,
    ada_weight,
    ada_bias,
    qkv_weight,
    query_value_bias,
    output_weight,
    output_bias,
    up_weight,
    up_bias,
    down_weight,
    down_bias,
):
    batches, images, rows = tokens.shape[:3]
    count = batches * images
    own = count // seq
    place = lax.axis_index("seq")
    index = lax.axis_index("grp")
    stages = group_stages(group)
    shifts = seq_shifts(seq)
    chunks = CHUNKS if sum(CHUNKS) == own else (own,)
    starts = [sum(chunks[:c]) for c in range(len(chunks))]
    whole = (tokens.reshape(count, rows, D), cotangent.reshape(count, rows, D))
    condition = condition.reshape(count, D)
    noise_levels = noise_levels.reshape(count)

    def pieces(chunk):
        return [
            jnp.stack([cut(array, ((place + shift) % seq) * own + starts[chunk], chunks[chunk]) for array in whole])
            for shift in shifts
        ]

    def fetch(sources):
        return [block if shift == 0 else seq_shift(block, shift, seq) for shift, block in zip(shifts, sources)]

    blocks = fetch(pieces(0))
    later = [pieces(chunk) for chunk in range(1, len(chunks))]

    flags = cut(mask_flags.reshape(count), place * own, own)
    sources = jnp.stack([(place - shift) % seq for shift in shifts])
    live = jnp.logical_or(flags[:, None] == 0, sources[None, :] * rows < KEEP).astype(jnp.float32)

    mine = cut(condition, place * own, own) + jnp.dot(
        level_rows(cut(noise_levels, place * own, own)), level_table, precision=highest
    )
    modulation = (
        jnp.dot(jax.nn.silu(mine).astype(jnp.bfloat16), ada_weight, preferred_element_type=jnp.float32) + ada_bias
    ).reshape(own, 6, D)

    bias_full = jnp.concatenate([query_value_bias[:D], jnp.zeros((D,), jnp.float32), query_value_bias[D:]])
    weights = (
        qkv_weight,
        output_weight,
        up_weight,
        down_weight,
        bias_full[None],
        output_bias[None],
        up_bias[None],
        down_bias[None],
    )
    high = mine.astype(jnp.bfloat16)
    own_levels = cut(noise_levels, place * own, own).astype(jnp.bfloat16)
    side = jnp.concatenate(
        [high, (mine - high.astype(jnp.float32)).astype(jnp.bfloat16), jnp.broadcast_to(own_levels[:, None], (own, 128))],
        1,
    )
    bit = stage_bit(stages[0], index)
    carried = None
    g_mods = []

    def give(buffer, shift, start, after, source=None):
        if shift != 0:
            buffer = seq_shift(tied(buffer, after), -shift, seq)
        start = ((place + (shift if source is None else source)) % seq) * own + start
        for k in range(2):
            targets[k] = lax.dynamic_update_slice_in_dim(targets[k], buffer[k], start, 0)
        return buffer

    def back(buffers, k, after):
        return seq_shift(tied(buffers[k], after), -shifts[k], seq) if k else buffers[0]

    def put(buffer, k, chunk):
        for which in range(2):
            targets[which] = lax.dynamic_update_slice_in_dim(
                targets[which], buffer[which], ((place + shifts[k]) % seq) * own + starts[chunk], 0
            )

    held = []
    released = None
    for chunk in range(len(chunks)):
        final = chunk + 1 == len(chunks)
        if chunk == 0:
            live, later = lax.optimization_barrier((live, later))
        following = None if final else fetch(tied(later[chunk], blocks))
        span = slice(starts[chunk], starts[chunk] + chunks[chunk])
        if final:
            early = [[back(buffers, k, (blocks, released)) for k in range(len(shifts))] for buffers in held[:-1]]
            ahead = [back(buffers, 2, (blocks, released)) for buffers in held[-1:]]
        buffers, g_mod, carried = layer_call(
            bit, live[span], blocks, modulation[span], weights, carried, None, 0, chunks[chunk], final, count
        )
        held.append(buffers)
        released = g_mod
        g_mods.append(g_mod)
        blocks = following

    keep, send, *targets, bias_sums = carried
    send = tied(send, (early, ahead))
    for chunk, buffers in enumerate(early):
        for k, buffer in enumerate(buffers):
            put(buffer, k, chunk)
    after = {}
    if len(chunks) > 1:
        middle = [ahead[0] if k == 2 else back(held[-2], k, early) for k in range(len(shifts))]
        after = {1: middle[3], len(stages): middle[1]}
        for k, buffer in enumerate(middle):
            put(buffer, k, len(chunks) - 2)
    part, given = scatter_grp(keep, send, index, stages, after)
    if len(stages) in after:
        part = tied(part, after[len(stages)])
    quarter = scatter_seq(part, place, seq)
    given += [part, quarter]
    part = gather_seq(quarter, place, seq, 1)
    bias_side = jnp.pad(bias_sums, ((0, 0), (0, own * SIDE - WIDE))).reshape(own, SIDE)
    small = jnp.concatenate(
        [jnp.concatenate([g.reshape(-1, 6 * D) for g in g_mods]).astype(jnp.bfloat16), bias_side.astype(jnp.bfloat16), side],
        1,
    )
    small = tied(small, given[1])
    given = iter(given[-1:] * (len(stages) - 1) + [part])
    for k in range(seq.bit_length() - 1):
        small = join_seq(small, place, 1 << k, seq)
    for step in group_steps(index, group):
        small = step(tied(small, next(given, part)))
    grad_ada, grad_ada_bias, bias_side, g_cond, grad_level = ada_call(small, ada_weight, own)
    final_rows = [back(held[-1], k, part) for k in range(len(shifts))]
    joins = list(reversed(stages[1:]))
    for k, stage in enumerate(joins):
        if k + 1 == len(joins):
            part = tied(part, (final_rows[1], final_rows[2], small))
        part = join(part, index, stage)
    part, grad_ada = lax.optimization_barrier((part, grad_ada))
    part = tied(part, final_rows[3])
    other = swap(part, stages[0])
    for k, buffer in enumerate(final_rows):
        put(buffer, k, len(chunks) - 1)
    grad_up, grad_down, grad_qkv, grad_out = finish(bit, part, other)

    grad_ada_bias = grad_ada_bias[0]
    bias_all = bias_side.reshape(own * SIDE)
    grad_condition = cut(g_cond, index * count, count)
    return (
        targets[0].reshape(batches, images, rows, D),
        targets[1].reshape(batches, images, rows, D),
        grad_condition.reshape(batches, images, D),
        grad_level,
        grad_ada,
        grad_ada_bias,
        grad_qkv,
        jnp.concatenate([bias_all[QKV : QKV + D], bias_all[QKV + 2 * D : QKV + 3 * D]]),
        grad_out,
        bias_all[OUT : OUT + D],
        grad_up,
        bias_all[UP : UP + FF],
        grad_down,
        bias_all[DOWN : DOWN + D],
    )


def solution(mesh):
    rows = P(None, "grp", "seq", None)
    in_specs = (rows, rows, P(None, "grp", None), P(None, "grp"), P(None, "grp")) + (P(),) * 11
    out_specs = (rows, rows, P(None, "grp", None)) + (P(),) * 11
    body = functools.partial(shards, mesh.shape["grp"], mesh.shape["seq"])
    return jax.shard_map(body, mesh=mesh, in_specs=in_specs, out_specs=out_specs, check_vma=False)
```

```python
import functools
import math

import jax
import jax.numpy as jnp
from jax import lax
from jax.experimental import pallas as pl
from jax.experimental.pallas import tpu as pltpu
from jax.sharding import PartitionSpec as P

D = 384
HEADS = 6
HEAD_DIM = 64
FF = 1536
SEQ_LEN = 256
KEEP = 128
LEVELS = 64
EPSILON = 1e-06
highest = lax.Precision.HIGHEST

UP, DOWN, QKV, OUT, WIDE = 0, FF, 2 * FF, 2 * FF + 3 * D, 2 * FF + 4 * D
FF_TILE = 1536
CHUNKS = (2, 3, 3)
SIDE = 640
COND = 6 * D + SIDE
LEVEL = COND + 2 * D
KERNEL_FLOPS = 30_000_000_000


def dot_nn(a, b):
    return lax.dot_general(a, b, (((1,), (0,)), ((), ())), preferred_element_type=jnp.float32)


def dot_nt(a, b):
    return lax.dot_general(a, b, (((1,), (1,)), ((), ())), preferred_element_type=jnp.float32)


def dot_tn(a, b):
    return lax.dot_general(a, b, (((0,), (0,)), ((), ())), preferred_element_type=jnp.float32)


def row_mean(values):
    return jnp.mean(values, -1, keepdims=True)


def layer_norm(values):
    centered = values - row_mean(values)
    rstd = lax.rsqrt(row_mean(centered * centered) + EPSILON)
    return centered * rstd, rstd


def norm_back(grad, normed, rstd):
    return rstd * (grad - row_mean(grad) - normed * row_mean(grad * normed))


def col_sum(values):
    return jnp.sum(values, 0, keepdims=True)


def layer_kernel(parts, first, last, placed, *refs):
    bit_ref, live_ref = refs[:2]
    refs = refs[1:]
    ins = refs[1 : 1 + parts]
    (mod_ref, wqkv, wout, wup, wdown, bqkv, bout, bup, bdown) = refs[1 + parts : 10 + parts]
    rest = refs[10 + parts :]
    if not first:
        acc_in, bias_in = rest[:2]
        rest = rest[2:]
    if placed:
        rest = rest[parts:]
    outs = rest[:parts]
    gmod_ref, bias_acc, acc_out = rest[parts : parts + 3]
    if last:
        give_out = rest[parts + 3]
        rest = rest[3:]
    acc, probs_ref, sem = rest[parts + 3 : parts + 6]
    acc_low = rest[parts + 6] if last else acc
    step = pl.program_id(0)
    steps = pl.num_programs(0)

    def send(start, stop, slot):
        @pl.when(step == steps - 1)
        def _():
            if last:
                low = bit_ref[0] == 0
                top = acc[: D // 2, start:stop].astype(jnp.bfloat16)
                bottom = acc[D // 2 :, start:stop].astype(jnp.bfloat16)
                acc_low[: D // 2, start:stop] = jnp.where(low, top, bottom)
                acc_low[D // 2 :, start:stop] = jnp.where(low, bottom, top)
            for copy in sent(start, stop, slot):
                copy.start()

    def sent(start, stop, slot):
        if not last:
            return [pltpu.make_async_copy(acc.at[:, start:stop], acc_out.at[:, start:stop], sem.at[slot])]
        return [
            pltpu.make_async_copy(
                acc_low.at[k * (D // 2) : (k + 1) * (D // 2), start:stop], out.at[:, start:stop], sem.at[2 * k + slot]
            )
            for k, out in enumerate((acc_out, give_out))
        ]

    @pl.when(step == 0)
    def _():
        if first:
            acc[...] = jnp.zeros_like(acc)
            bias_acc[...] = jnp.zeros_like(bias_acc)
        else:
            pltpu.make_async_copy(acc_in, acc, sem.at[0]).start()
            bias_acc[...] = bias_in[...]

    rows = ins[0].shape[2]
    full = parts * rows
    tokens = jnp.concatenate([ref[0, 0] for ref in ins], 0).astype(jnp.float32)
    live_parts = [live_ref[step, p] for p in range(parts)]
    live = jnp.concatenate([jnp.full((rows, 1), flag, jnp.float32) for flag in live_parts], 0)
    key_part = lax.broadcasted_iota(jnp.int32, (1, full), 1) // rows
    live_keys = jnp.zeros((1, full), jnp.float32)
    for p in range(parts):
        live_keys = jnp.where(key_part == p, live_parts[p], live_keys)
    live_keys = live_keys > 0.5
    mod = mod_ref[0]
    shift_one, scale_one, gate_one = mod[0:1], 1.0 + mod[1:2], mod[2:3]
    shift_two, scale_two, gate_two = mod[3:4], 1.0 + mod[4:5], mod[5:6]

    norm_one, rstd_one = layer_norm(tokens)
    in_one = (norm_one * scale_one + shift_one).astype(jnp.bfloat16)
    projected = dot_nn(in_one, wqkv[...]) + bqkv[...]
    inv_root = 1.0 / math.sqrt(HEAD_DIM)
    queries = (projected[:, :D].astype(jnp.bfloat16) * jnp.bfloat16(inv_root)).astype(jnp.bfloat16)
    keys = projected[:, D : 2 * D].astype(jnp.bfloat16)
    values = projected[:, 2 * D :].astype(jnp.bfloat16)
    lanes = lax.broadcasted_iota(jnp.int32, (1, 2 * HEAD_DIM), 1)
    halves = (lanes < HEAD_DIM, lanes >= HEAD_DIM)

    def pair(array, j):
        return array[:, j * 2 * HEAD_DIM : (j + 1) * 2 * HEAD_DIM]

    def half(array, h):
        return jnp.where(halves[h], array, jnp.zeros_like(array))

    def head_scores(n):
        j, h = divmod(n, 2)
        return jnp.where(live_keys, dot_nt(pair(queries, j), half(pair(keys, j), h)), -1e30)

    attended = []
    every = [head_scores(n) for n in range(HEADS)]
    for n in range(HEADS):
        scores, ahead = every[n], None
        j, h = divmod(n, 2)
        exps = jnp.exp(scores - jnp.max(scores, -1, keepdims=True))
        probs = exps * (1.0 / jnp.sum(exps, -1, keepdims=True))
        probs_ref[n] = probs
        term = dot_nn(probs.astype(jnp.bfloat16), half(pair(values, j), h))
        if h == 0:
            total = term
        else:
            attended.append((total + term).astype(jnp.bfloat16))
        scores = ahead
    attended = jnp.concatenate(attended, 1)
    attn_branch = dot_nn(attended, wout[...]) + bout[...]
    live_gate_one = live * gate_one
    residual = tokens + live_gate_one * attn_branch
    norm_two, rstd_two = layer_norm(residual)
    in_two = (norm_two * scale_two + shift_two).astype(jnp.bfloat16)

    g_output = jnp.concatenate([ref[1, 0] for ref in ins], 0).astype(jnp.float32)
    live_out = live * g_output
    g_ffn = (live_out * gate_two).astype(jnp.bfloat16)
    if not first:

        @pl.when(step == 0)
        def _():
            pltpu.make_async_copy(acc_in, acc, sem.at[0]).wait()

    in_two_t = in_two.T
    g_ffn_t = g_ffn.T
    ffn = None
    g_in_two = None
    root = math.sqrt(2.0 / math.pi)
    for tile in range(FF // FF_TILE):
        cols = slice(tile * FF_TILE, (tile + 1) * FF_TILE)
        pre = dot_nn(in_two, wup[:, cols]) + bup[:, cols]
        square = pre * pre
        gate = 0.5 + 0.5 * jnp.tanh(pre * (root + (root * 0.044715) * square))
        hidden_wide = pre * gate
        slope = gate + hidden_wide * (1.0 - gate) * (2.0 * root + (6.0 * root * 0.044715) * square)
        hidden = hidden_wide.astype(jnp.bfloat16)
        term = dot_nn(hidden, wdown[cols, :])
        ffn = term if ffn is None else ffn + term
        g_pre_wide = dot_nt(g_ffn, wdown[cols, :]) * slope
        g_pre = g_pre_wide.astype(jnp.bfloat16)
        acc[:, DOWN + tile * FF_TILE : DOWN + (tile + 1) * FF_TILE] += dot_nn(g_ffn_t, hidden)
        acc[:, UP + tile * FF_TILE : UP + (tile + 1) * FF_TILE] += dot_nn(in_two_t, g_pre)
        bias_acc[:, UP + tile * FF_TILE : UP + (tile + 1) * FF_TILE] += col_sum(g_pre.astype(jnp.float32))
        term = dot_nt(g_pre, wup[:, cols])
        g_in_two = term if g_in_two is None else g_in_two + term
    send(UP, QKV, 0)
    bias_acc[:, DOWN : DOWN + D] += col_sum(g_ffn.astype(jnp.float32))
    ffn = ffn + bdown[...]
    layer_out = (residual + live * gate_two * ffn).astype(jnp.bfloat16)
    for p in range(parts):
        outs[p][0, 0] = layer_out[p * rows : (p + 1) * rows]
    gmod_ref[0, 5:6] = col_sum(live_out * ffn)
    gmod_ref[0, 4:5] = col_sum(g_in_two * norm_two)
    gmod_ref[0, 3:4] = col_sum(g_in_two)
    g_residual = g_output + norm_back(g_in_two * scale_two, norm_two, rstd_two)
    g_attn = (live_gate_one * g_residual).astype(jnp.bfloat16)
    gmod_ref[0, 2:3] = col_sum(live * g_residual * attn_branch)
    acc[:, OUT : OUT + D] += dot_tn(attended, g_attn)
    bias_acc[:, OUT : OUT + D] += col_sum(g_attn.astype(jnp.float32))
    g_attended = dot_nt(g_attn, wout[...]).astype(jnp.bfloat16)

    g_queries, g_keys, g_values = [], [], []

    def head_probs(n):
        j, h = divmod(n, 2)
        return dot_nt(pair(g_attended, j), half(pair(values, j), h))

    queries_t = queries.T
    g_attended_t = g_attended.T
    every = [head_probs(n) for n in range(HEADS)]
    for n in range(HEADS):
        j, h = divmod(n, 2)
        head = slice(n * HEAD_DIM, (n + 1) * HEAD_DIM)
        probs = probs_ref[n]
        weighted = probs * every[n]
        g_scores = (weighted - probs * jnp.sum(weighted, -1, keepdims=True)).astype(jnp.bfloat16)
        tq = dot_nn(g_scores, half(pair(keys, j), h))
        g_keys.append(dot_nn(queries_t[head], g_scores).astype(jnp.bfloat16))
        g_values.append(dot_nn(g_attended_t[head], probs.astype(jnp.bfloat16)).astype(jnp.bfloat16))
        if h == 0:
            gq = tq
        else:
            g_queries.append(((gq + tq) * inv_root).astype(jnp.bfloat16))
    g_keys = [jnp.concatenate(g_keys, 0).T]
    g_values = [jnp.concatenate(g_values, 0).T]
    g_projected = jnp.concatenate(g_queries + g_keys + g_values, 1)
    acc[:, QKV : QKV + 3 * D] += dot_tn(in_one, g_projected)
    send(QKV, WIDE, 1)
    bias_acc[:, QKV : QKV + 3 * D] += col_sum(g_projected.astype(jnp.float32))
    g_in_one = dot_nt(g_projected, wqkv[...])
    gmod_ref[0, 1:2] = col_sum(g_in_one * norm_one)
    gmod_ref[0, 0:1] = col_sum(g_in_one)
    g_tokens = (g_residual + norm_back(g_in_one * scale_one, norm_one, rstd_one)).astype(jnp.bfloat16)
    for p in range(parts):
        outs[p][1, 0] = g_tokens[p * rows : (p + 1) * rows]

    @pl.when(step == steps - 1)
    def _():
        for copy in sent(UP, QKV, 0) + sent(QKV, WIDE, 1):
            copy.wait()


def layer_call(bit, live, blocks, mod, weights, carried, buffers, place, size, last, room):
    parts = len(blocks)
    images, rows = blocks[0].shape[1:3]
    first = carried is None
    resident = [pl.BlockSpec(w.shape, lambda i: (0, 0), pipeline_mode=pl.Buffered(1)) for w in weights]
    block_spec = pl.BlockSpec((2, 1, rows, D), lambda i: (0, i, 0, 0))
    out_spec = pl.BlockSpec((2, 1, rows, D), lambda i: (0, i + place, 0, 0))
    mod_spec = pl.BlockSpec((1, 6, D), lambda i: (i, 0, 0))
    any_spec = pl.BlockSpec(memory_space=pl.ANY)
    bias_spec = pl.BlockSpec((1, WIDE), lambda i: (0, 0))
    in_specs = (
        [pl.BlockSpec(memory_space=pltpu.SMEM)] * 2 + [block_spec] * parts + [mod_spec] + resident
    )
    args = [bit.reshape(1), live, *blocks, mod, *weights]
    aliases = {}
    if not first:
        in_specs += [any_spec, bias_spec]
        if not last:
            aliases[len(args)] = parts + 2
        args += list(carried)
    if buffers is not None:
        in_specs += [any_spec] * parts
        aliases.update({len(args) + p: p for p in range(parts)})
        args += list(buffers)
    if last:
        sums = [jax.ShapeDtypeStruct((D // 2, WIDE), jnp.bfloat16)] * 2
        sums += [jax.ShapeDtypeStruct((room, rows, D), jnp.bfloat16)] * 2
    else:
        sums = [jax.ShapeDtypeStruct((D, WIDE), jnp.float32)]
    scratch = [
        pltpu.VMEM((D, WIDE), jnp.float32),
        pltpu.VMEM((HEADS, parts * rows, parts * rows), jnp.float32),
        pltpu.SemaphoreType.DMA((4,)),
    ]
    if last:
        scratch.append(pltpu.VMEM((D, WIDE), jnp.bfloat16))
    result = pl.pallas_call(
        functools.partial(layer_kernel, parts, first, last, buffers is not None),
        grid=(images,),
        in_specs=in_specs,
        out_specs=[out_spec] * parts + [mod_spec, bias_spec] + [any_spec] * len(sums),
        out_shape=[jax.ShapeDtypeStruct((2, size, rows, D), jnp.bfloat16)] * parts
        + [
            jax.ShapeDtypeStruct((images, 6, D), jnp.float32),
            jax.ShapeDtypeStruct((1, WIDE), jnp.float32),
        ]
        + sums,
        scratch_shapes=scratch,
        input_output_aliases=aliases,
        cost_estimate=pl.CostEstimate(
            flops=KERNEL_FLOPS * images, transcendentals=0, bytes_accessed=8 * images * parts * rows * D
        ),
        compiler_params=pltpu.CompilerParams(vmem_limit_bytes=52 * 1024 * 1024),
    )(*args)
    return result[:parts], result[parts], (*result[parts + 2 :], result[parts + 1])


def finish_kernel(bit_ref, mine_ref, other_ref, up_ref, down_ref, qkv_ref, out_ref):
    low = bit_ref[0] == 0
    size = mine_ref.shape[0]
    mine, other = mine_ref[...], other_ref[...]
    down = []
    for k in range(2):
        part = jnp.where(low, mine, other) if k == 0 else jnp.where(low, other, mine)
        span = slice(k * size, (k + 1) * size)
        up_ref[span] = part[:, UP : UP + FF].astype(jnp.float32)
        qkv_ref[span] = part[:, QKV : QKV + 3 * D].astype(jnp.float32)
        out_ref[span] = part[:, OUT : OUT + D].astype(jnp.float32)
        down.append(part[:, DOWN : DOWN + FF])
    down_ref[...] = jnp.concatenate(down, 0).T.astype(jnp.float32)


def finish(bit, mine, other):
    full = pl.BlockSpec(memory_space=pltpu.VMEM)
    rows = 2 * mine.shape[0]
    shapes = [(rows, FF), (FF, rows), (rows, 3 * D), (rows, D)]
    return pl.pallas_call(
        finish_kernel,
        in_specs=[pl.BlockSpec(memory_space=pltpu.SMEM), full, full],
        out_specs=[full] * 4,
        out_shape=[jax.ShapeDtypeStruct(shape, jnp.float32) for shape in shapes],
        compiler_params=pltpu.CompilerParams(vmem_limit_bytes=52 * 1024 * 1024),
    )(bit.reshape(1), mine, other)


def ada_kernel(small_ref, weight_ref, grad_ref, bias_ref, side_ref, cond_out, level_ref):
    rows = small_ref.shape[0]
    small = small_ref[:, : 6 * D]
    slot = lax.broadcasted_iota(jnp.int32, (side_ref.shape[0], rows), 0)
    row = lax.broadcasted_iota(jnp.int32, (side_ref.shape[0], rows), 1)
    picks = (row % side_ref.shape[0] == slot).astype(jnp.bfloat16)
    bias_ref[...] = col_sum(dot_nn(picks, small))
    side_ref[...] = dot_nn(picks, small_ref[:, 6 * D : COND])
    cond = small_ref[:, COND : COND + D].astype(jnp.float32) + small_ref[:, COND + D : LEVEL].astype(jnp.float32)
    gate = jax.nn.sigmoid(cond)
    g_cond = dot_nt(small, weight_ref[...]) * (gate * (1.0 + cond * (1.0 - gate)))
    cond_out[...] = g_cond
    levels = small_ref[:, LEVEL : LEVEL + 128].astype(jnp.float32)
    onehot = (levels == lax.broadcasted_iota(jnp.int32, (rows, 128), 1).astype(jnp.float32)).astype(jnp.float32)
    level_ref[...] = lax.dot_general(
        onehot, g_cond, (((0,), (0,)), ((), ())), precision=highest, preferred_element_type=jnp.float32
    )[:LEVELS]
    grad_ref[...] = dot_tn((cond * gate).astype(jnp.bfloat16), small)


def ada_call(small, weight, own):
    full = pl.BlockSpec(memory_space=pltpu.VMEM)
    rows = small.shape[0]
    shapes = [(D, 6 * D), (1, 6 * D), (own, SIDE), (rows, D), (LEVELS, D)]
    return pl.pallas_call(
        ada_kernel,
        in_specs=[full] * 2,
        out_specs=[full] * 5,
        out_shape=[jax.ShapeDtypeStruct(shape, jnp.float32) for shape in shapes],
        cost_estimate=pl.CostEstimate(flops=6_000_000_000, transcendentals=0, bytes_accessed=8_000_000),
        compiler_params=pltpu.CompilerParams(vmem_limit_bytes=52 * 1024 * 1024),
    )(small, weight)


def cut(array, start, size, axis=0):
    return lax.dynamic_slice_in_dim(array, start, size, axis)


def group_stages(size):
    bits = [1 << k for k in range(size.bit_length() - 1)]
    if size == 8:
        table = [[1] * 8, [2 if i % 2 == 0 else 4 for i in range(8)], [4 if i % 2 == 0 else 2 for i in range(8)]]
    else:
        table = [[bit] * size for bit in bits]
    return table


def stage_bit(stage, index):
    masks = jnp.asarray(stage, jnp.int32)[index] if len(set(stage)) > 1 else stage[0]
    return jnp.where((index & masks) != 0, 1, 0)


def swap(array, stage):
    return lax.ppermute(array, "grp", [(i, i ^ bit) for i, bit in enumerate(stage)])


def seq_shift(array, shift, size):
    return lax.ppermute(array, "seq", [(i, (i + shift) % size) for i in range(size)])


def scatter_grp(keep, give, index, stages, after):
    given = []
    for k, stage in enumerate(stages):
        if k in after:
            give = tied(give, after[k])
        given.append(give)
        got = swap(give, stage)
        if k + 1 < len(stages):
            size = keep.shape[0] // 2
            bit = stage_bit(stages[k + 1], index)
            keep, give = [
                (cut(keep, b * size, size).astype(jnp.float32) + cut(got, b * size, size).astype(jnp.float32)).astype(
                    jnp.bfloat16
                )
                for b in (bit, 1 - bit)
            ]
    return (keep.astype(jnp.float32) + got.astype(jnp.float32)).astype(jnp.bfloat16), given


def scatter_seq(array, place, seq):
    size = array.shape[1] // seq
    total = cut(array, place * size, size, 1).astype(jnp.float32)
    for shift in seq_shifts(seq)[1:]:
        total = total + seq_shift(cut(array, ((place + shift) % seq) * size, size, 1), shift, seq).astype(jnp.float32)
    return total.astype(jnp.bfloat16)


def gather_seq(array, place, seq, axis):
    size = array.shape[axis]
    shape = list(array.shape)
    shape[axis] = size * seq
    whole = lax.dynamic_update_slice_in_dim(jnp.zeros(shape, array.dtype), array, place * size, axis)
    for shift in seq_shifts(seq)[1:]:
        got = seq_shift(array, shift, seq)
        whole = lax.dynamic_update_slice_in_dim(whole, got, ((place - shift) % seq) * size, axis)
    return whole


def join(array, index, stage):
    got = swap(array, stage)
    low = stage_bit(stage, index) == 0
    return jnp.where(low, jnp.concatenate([array, got], 0), jnp.concatenate([got, array], 0))


def join_seq(array, place, bit, seq):
    got = lax.ppermute(array, "seq", [(i, i ^ bit) for i in range(seq)])
    low = (place & bit) == 0
    return jnp.where(low, jnp.concatenate([array, got], 0), jnp.concatenate([got, array], 0))


def join_last(array, index, stage):
    got = swap(array, stage)
    low = stage_bit(stage, index) == 0
    first, second = jnp.where(low, array, got), jnp.where(low, got, array)
    half = first.shape[0] // 2
    odd = (index & 1) == 0
    return jnp.concatenate(
        [
            first[:half],
            jnp.where(odd, second[:half], first[half:]),
            jnp.where(odd, first[half:], second[:half]),
            second[half:],
        ],
        0,
    )


def group_steps(index, group):
    stages = group_stages(group)
    if group == 8:
        stages[1:] = stages[:0:-1]
    steps = [functools.partial(join, index=index, stage=stage) for stage in stages]
    if group == 8:
        steps[-1] = functools.partial(join_last, index=index, stage=stages[-1])
    return steps


def seq_shifts(seq):
    return (0, 2, 1, 3) if seq == 4 else tuple(range(seq))


def tied(values, after):
    return lax.optimization_barrier((values, after))[0]


def level_rows(levels):
    return (levels[:, None] == jnp.arange(LEVELS, dtype=levels.dtype)[None, :]).astype(jnp.float32)


def shards(
    group,
    seq,
    tokens,
    cotangent,
    condition,
    mask_flags,
    noise_levels,
    level_table,
    ada_weight,
    ada_bias,
    qkv_weight,
    query_value_bias,
    output_weight,
    output_bias,
    up_weight,
    up_bias,
    down_weight,
    down_bias,
):
    batches, images, rows = tokens.shape[:3]
    count = batches * images
    own = count // seq
    place = lax.axis_index("seq")
    index = lax.axis_index("grp")
    stages = group_stages(group)
    shifts = seq_shifts(seq)
    chunks = CHUNKS if sum(CHUNKS) == own else (own,)
    starts = [sum(chunks[:c]) for c in range(len(chunks))]
    whole = (tokens.reshape(count, rows, D), cotangent.reshape(count, rows, D))
    condition = condition.reshape(count, D)
    noise_levels = noise_levels.reshape(count)

    def pieces(chunk):
        return [
            jnp.stack([cut(array, ((place + shift) % seq) * own + starts[chunk], chunks[chunk]) for array in whole])
            for shift in shifts
        ]

    def fetch(sources):
        return [block if shift == 0 else seq_shift(block, shift, seq) for shift, block in zip(shifts, sources)]

    blocks = fetch(pieces(0))
    later = [pieces(chunk) for chunk in range(1, len(chunks))]

    flags = cut(mask_flags.reshape(count), place * own, own)
    sources = jnp.stack([(place - shift) % seq for shift in shifts])
    live = jnp.logical_or(flags[:, None] == 0, sources[None, :] * rows < KEEP).astype(jnp.float32)

    mine = cut(condition, place * own, own) + jnp.dot(
        level_rows(cut(noise_levels, place * own, own)), level_table, precision=highest
    )
    modulation = (
        jnp.dot(jax.nn.silu(mine).astype(jnp.bfloat16), ada_weight, preferred_element_type=jnp.float32) + ada_bias
    ).reshape(own, 6, D)

    bias_full = jnp.concatenate([query_value_bias[:D], jnp.zeros((D,), jnp.float32), query_value_bias[D:]])
    weights = (
        qkv_weight,
        output_weight,
        up_weight,
        down_weight,
        bias_full[None],
        output_bias[None],
        up_bias[None],
        down_bias[None],
    )
    high = mine.astype(jnp.bfloat16)
    own_levels = cut(noise_levels, place * own, own).astype(jnp.bfloat16)
    side = jnp.concatenate(
        [high, (mine - high.astype(jnp.float32)).astype(jnp.bfloat16), jnp.broadcast_to(own_levels[:, None], (own, 128))],
        1,
    )
    bit = stage_bit(stages[0], index)
    carried = None
    g_mods = []

    def give(buffer, shift, start, after, source=None):
        if shift != 0:
            buffer = seq_shift(tied(buffer, after), -shift, seq)
        start = ((place + (shift if source is None else source)) % seq) * own + start
        for k in range(2):
            targets[k] = lax.dynamic_update_slice_in_dim(targets[k], buffer[k], start, 0)
        return buffer

    def back(buffers, k, after):
        return seq_shift(tied(buffers[k], after), -shifts[k], seq) if k else buffers[0]

    def put(buffer, k, chunk):
        for which in range(2):
            targets[which] = lax.dynamic_update_slice_in_dim(
                targets[which], buffer[which], ((place + shifts[k]) % seq) * own + starts[chunk], 0
            )

    held = []
    released = None
    for chunk in range(len(chunks)):
        final = chunk + 1 == len(chunks)
        if chunk == 0:
            live, later = lax.optimization_barrier((live, later))
        following = None if final else fetch(tied(later[chunk], blocks))
        span = slice(starts[chunk], starts[chunk] + chunks[chunk])
        if final:
            early = [[back(buffers, k, (blocks, released)) for k in range(len(shifts))] for buffers in held[:-1]]
            ahead = [back(buffers, 2, (blocks, released)) for buffers in held[-1:]]
        buffers, g_mod, carried = layer_call(
            bit, live[span], blocks, modulation[span], weights, carried, None, 0, chunks[chunk], final, count
        )
        held.append(buffers)
        released = g_mod
        g_mods.append(g_mod)
        blocks = following

    keep, send, *targets, bias_sums = carried
    send = tied(send, (early, ahead))
    for chunk, buffers in enumerate(early):
        for k, buffer in enumerate(buffers):
            put(buffer, k, chunk)
    after = {}
    if len(chunks) > 1:
        middle = [ahead[0] if k == 2 else back(held[-2], k, early) for k in range(len(shifts))]
        after = {len(stages): (middle[1], middle[3])}
        for k, buffer in enumerate(middle):
            put(buffer, k, len(chunks) - 2)
    part, given = scatter_grp(keep, send, index, stages, after)
    if len(stages) in after:
        part = tied(part, after[len(stages)])
    quarter = scatter_seq(part, place, seq)
    given += [part, quarter]
    part = gather_seq(quarter, place, seq, 1)
    bias_side = jnp.pad(bias_sums, ((0, 0), (0, own * SIDE - WIDE))).reshape(own, SIDE)
    small = jnp.concatenate(
        [jnp.concatenate([g.reshape(-1, 6 * D) for g in g_mods]).astype(jnp.bfloat16), bias_side.astype(jnp.bfloat16), side],
        1,
    )
    small = tied(small, given[1])
    given = iter([given[-2]] + given[-1:] * (len(stages) - 2) + [part])
    for k in range(seq.bit_length() - 1):
        small = join_seq(small, place, 1 << k, seq)
    for step in group_steps(index, group):
        small = step(tied(small, next(given, part)))
    grad_ada, grad_ada_bias, bias_side, g_cond, grad_level = ada_call(small, ada_weight, own)
    final_rows = [back(held[-1], k, part) for k in range(len(shifts))]
    joins = list(reversed(stages[1:]))
    for k, stage in enumerate(joins):
        if k + 1 == len(joins):
            part = tied(part, (final_rows[1], final_rows[2], small))
        part = join(part, index, stage)
    part, grad_ada = lax.optimization_barrier((part, grad_ada))
    part = tied(part, final_rows[3])
    other = swap(part, stages[0])
    for k, buffer in enumerate(final_rows):
        put(buffer, k, len(chunks) - 1)
    grad_up, grad_down, grad_qkv, grad_out = finish(bit, part, other)

    grad_ada_bias = grad_ada_bias[0]
    bias_all = bias_side.reshape(own * SIDE)
    grad_condition = cut(g_cond, index * count, count)
    return (
        targets[0].reshape(batches, images, rows, D),
        targets[1].reshape(batches, images, rows, D),
        grad_condition.reshape(batches, images, D),
        grad_level,
        grad_ada,
        grad_ada_bias,
        grad_qkv,
        jnp.concatenate([bias_all[QKV : QKV + D], bias_all[QKV + 2 * D : QKV + 3 * D]]),
        grad_out,
        bias_all[OUT : OUT + D],
        grad_up,
        bias_all[UP : UP + FF],
        grad_down,
        bias_all[DOWN : DOWN + D],
    )


def solution(mesh):
    rows = P(None, "grp", "seq", None)
    in_specs = (rows, rows, P(None, "grp", None), P(None, "grp"), P(None, "grp")) + (P(),) * 11
    out_specs = (rows, rows, P(None, "grp", None)) + (P(),) * 11
    body = functools.partial(shards, mesh.shape["grp"], mesh.shape["seq"])
    return jax.shard_map(body, mesh=mesh, in_specs=in_specs, out_specs=out_specs, check_vma=False)
```

```python
import functools
import math

import jax
import jax.numpy as jnp
from jax import lax
from jax.experimental import pallas as pl
from jax.experimental.pallas import tpu as pltpu
from jax.sharding import PartitionSpec as P

D = 384
HEADS = 6
HEAD_DIM = 64
FF = 1536
SEQ_LEN = 256
KEEP = 128
LEVELS = 64
EPSILON = 1e-06
highest = lax.Precision.HIGHEST

UP, DOWN, QKV, OUT, WIDE = 0, FF, 2 * FF, 2 * FF + 3 * D, 2 * FF + 4 * D
FF_TILE = 1536
CHUNKS = (2, 3, 3)
SIDE = 640
COND = 6 * D + SIDE
LEVEL = COND + 2 * D
KERNEL_FLOPS = 30_000_000_000


def dot_nn(a, b):
    return lax.dot_general(a, b, (((1,), (0,)), ((), ())), preferred_element_type=jnp.float32)


def dot_nt(a, b):
    return lax.dot_general(a, b, (((1,), (1,)), ((), ())), preferred_element_type=jnp.float32)


def dot_tn(a, b):
    return lax.dot_general(a, b, (((0,), (0,)), ((), ())), preferred_element_type=jnp.float32)


def row_mean(values):
    return jnp.mean(values, -1, keepdims=True)


def layer_norm(values):
    centered = values - row_mean(values)
    rstd = lax.rsqrt(row_mean(centered * centered) + EPSILON)
    return centered * rstd, rstd


def norm_back(grad, normed, rstd):
    return rstd * (grad - row_mean(grad) - normed * row_mean(grad * normed))


def col_sum(values):
    return jnp.sum(values, 0, keepdims=True)


def layer_kernel(parts, first, last, placed, *refs):
    bit_ref, live_ref = refs[:2]
    refs = refs[1:]
    ins = refs[1 : 1 + parts]
    (mod_ref, wqkv, wout, wup, wdown, bqkv, bout, bup, bdown) = refs[1 + parts : 10 + parts]
    rest = refs[10 + parts :]
    if not first:
        acc_in, bias_in = rest[:2]
        rest = rest[2:]
    if placed:
        rest = rest[parts:]
    outs = rest[:parts]
    gmod_ref, bias_acc, acc_out = rest[parts : parts + 3]
    if last:
        give_out = rest[parts + 3]
        rest = rest[3:]
    acc, probs_ref, sem = rest[parts + 3 : parts + 6]
    acc_low = rest[parts + 6] if last else acc
    step = pl.program_id(0)
    steps = pl.num_programs(0)

    def send(start, stop, slot):
        @pl.when(step == steps - 1)
        def _():
            if last:
                low = bit_ref[0] == 0
                top = acc[: D // 2, start:stop].astype(jnp.bfloat16)
                bottom = acc[D // 2 :, start:stop].astype(jnp.bfloat16)
                acc_low[: D // 2, start:stop] = jnp.where(low, top, bottom)
                acc_low[D // 2 :, start:stop] = jnp.where(low, bottom, top)
            for copy in sent(start, stop, slot):
                copy.start()

    def sent(start, stop, slot):
        if not last:
            return [pltpu.make_async_copy(acc.at[:, start:stop], acc_out.at[:, start:stop], sem.at[slot])]
        return [
            pltpu.make_async_copy(
                acc_low.at[k * (D // 2) : (k + 1) * (D // 2), start:stop], out.at[:, start:stop], sem.at[2 * k + slot]
            )
            for k, out in enumerate((acc_out, give_out))
        ]

    @pl.when(step == 0)
    def _():
        if first:
            acc[...] = jnp.zeros_like(acc)
            bias_acc[...] = jnp.zeros_like(bias_acc)
        else:
            pltpu.make_async_copy(acc_in, acc, sem.at[0]).start()
            bias_acc[...] = bias_in[...]

    rows = ins[0].shape[2]
    full = parts * rows
    tokens = jnp.concatenate([ref[0, 0] for ref in ins], 0).astype(jnp.float32)
    live_parts = [live_ref[step, p] for p in range(parts)]
    live = jnp.concatenate([jnp.full((rows, 1), flag, jnp.float32) for flag in live_parts], 0)
    key_part = lax.broadcasted_iota(jnp.int32, (1, full), 1) // rows
    live_keys = jnp.zeros((1, full), jnp.float32)
    for p in range(parts):
        live_keys = jnp.where(key_part == p, live_parts[p], live_keys)
    live_keys = live_keys > 0.5
    mod = mod_ref[0]
    shift_one, scale_one, gate_one = mod[0:1], 1.0 + mod[1:2], mod[2:3]
    shift_two, scale_two, gate_two = mod[3:4], 1.0 + mod[4:5], mod[5:6]

    norm_one, rstd_one = layer_norm(tokens)
    in_one = (norm_one * scale_one + shift_one).astype(jnp.bfloat16)
    projected = dot_nn(in_one, wqkv[...]) + bqkv[...]
    inv_root = 1.0 / math.sqrt(HEAD_DIM)
    queries = (projected[:, :D].astype(jnp.bfloat16) * jnp.bfloat16(inv_root)).astype(jnp.bfloat16)
    keys = projected[:, D : 2 * D].astype(jnp.bfloat16)
    values = projected[:, 2 * D :].astype(jnp.bfloat16)
    lanes = lax.broadcasted_iota(jnp.int32, (1, 2 * HEAD_DIM), 1)
    halves = (lanes < HEAD_DIM, lanes >= HEAD_DIM)

    def pair(array, j):
        return array[:, j * 2 * HEAD_DIM : (j + 1) * 2 * HEAD_DIM]

    def half(array, h):
        return jnp.where(halves[h], array, jnp.zeros_like(array))

    def head_scores(n):
        j, h = divmod(n, 2)
        return jnp.where(live_keys, dot_nt(pair(queries, j), half(pair(keys, j), h)), -1e30)

    attended = []
    every = [head_scores(n) for n in range(HEADS)]
    for n in range(HEADS):
        scores, ahead = every[n], None
        j, h = divmod(n, 2)
        exps = jnp.exp(scores - jnp.max(scores, -1, keepdims=True))
        probs = exps * (1.0 / jnp.sum(exps, -1, keepdims=True))
        probs_ref[n] = probs
        term = dot_nn(probs.astype(jnp.bfloat16), half(pair(values, j), h))
        if h == 0:
            total = term
        else:
            attended.append((total + term).astype(jnp.bfloat16))
        scores = ahead
    attended = jnp.concatenate(attended, 1)
    attn_branch = dot_nn(attended, wout[...]) + bout[...]
    live_gate_one = live * gate_one
    residual = tokens + live_gate_one * attn_branch
    norm_two, rstd_two = layer_norm(residual)
    in_two = (norm_two * scale_two + shift_two).astype(jnp.bfloat16)

    g_output = jnp.concatenate([ref[1, 0] for ref in ins], 0).astype(jnp.float32)
    live_out = live * g_output
    g_ffn = (live_out * gate_two).astype(jnp.bfloat16)
    if not first:

        @pl.when(step == 0)
        def _():
            pltpu.make_async_copy(acc_in, acc, sem.at[0]).wait()

    in_two_t = in_two.T
    g_ffn_t = g_ffn.T
    ffn = None
    g_in_two = None
    root = math.sqrt(2.0 / math.pi)
    for tile in range(FF // FF_TILE):
        cols = slice(tile * FF_TILE, (tile + 1) * FF_TILE)
        pre = dot_nn(in_two, wup[:, cols]) + bup[:, cols]
        square = pre * pre
        gate = 0.5 + 0.5 * jnp.tanh(pre * (root + (root * 0.044715) * square))
        hidden_wide = pre * gate
        slope = gate + hidden_wide * (1.0 - gate) * (2.0 * root + (6.0 * root * 0.044715) * square)
        hidden = hidden_wide.astype(jnp.bfloat16)
        term = dot_nn(hidden, wdown[cols, :])
        ffn = term if ffn is None else ffn + term
        g_pre_wide = dot_nt(g_ffn, wdown[cols, :]) * slope
        g_pre = g_pre_wide.astype(jnp.bfloat16)
        acc[:, DOWN + tile * FF_TILE : DOWN + (tile + 1) * FF_TILE] += dot_nn(g_ffn_t, hidden)
        acc[:, UP + tile * FF_TILE : UP + (tile + 1) * FF_TILE] += dot_nn(in_two_t, g_pre)
        bias_acc[:, UP + tile * FF_TILE : UP + (tile + 1) * FF_TILE] += col_sum(g_pre.astype(jnp.float32))
        term = dot_nt(g_pre, wup[:, cols])
        g_in_two = term if g_in_two is None else g_in_two + term
    send(UP, QKV, 0)
    bias_acc[:, DOWN : DOWN + D] += col_sum(g_ffn.astype(jnp.float32))
    ffn = ffn + bdown[...]
    layer_out = (residual + live * gate_two * ffn).astype(jnp.bfloat16)
    for p in range(parts):
        outs[p][0, 0] = layer_out[p * rows : (p + 1) * rows]
    gmod_ref[0, 5:6] = col_sum(live_out * ffn)
    gmod_ref[0, 4:5] = col_sum(g_in_two * norm_two)
    gmod_ref[0, 3:4] = col_sum(g_in_two)
    g_residual = g_output + norm_back(g_in_two * scale_two, norm_two, rstd_two)
    g_attn = (live_gate_one * g_residual).astype(jnp.bfloat16)
    gmod_ref[0, 2:3] = col_sum(live * g_residual * attn_branch)
    acc[:, OUT : OUT + D] += dot_tn(attended, g_attn)
    bias_acc[:, OUT : OUT + D] += col_sum(g_attn.astype(jnp.float32))
    g_attended = dot_nt(g_attn, wout[...]).astype(jnp.bfloat16)

    g_queries, g_keys, g_values = [], [], []

    def head_probs(n):
        j, h = divmod(n, 2)
        return dot_nt(pair(g_attended, j), half(pair(values, j), h))

    queries_t = queries.T
    g_attended_t = g_attended.T
    every = [head_probs(n) for n in range(HEADS)]
    for n in range(HEADS):
        j, h = divmod(n, 2)
        head = slice(n * HEAD_DIM, (n + 1) * HEAD_DIM)
        probs = probs_ref[n]
        weighted = probs * every[n]
        g_scores = (weighted - probs * jnp.sum(weighted, -1, keepdims=True)).astype(jnp.bfloat16)
        tq = dot_nn(g_scores, half(pair(keys, j), h))
        g_keys.append(dot_nn(queries_t[head], g_scores).astype(jnp.bfloat16))
        g_values.append(dot_nn(g_attended_t[head], probs.astype(jnp.bfloat16)).astype(jnp.bfloat16))
        if h == 0:
            gq = tq
        else:
            g_queries.append(((gq + tq) * inv_root).astype(jnp.bfloat16))
    g_keys = [jnp.concatenate(g_keys, 0).T]
    g_values = [jnp.concatenate(g_values, 0).T]
    g_projected = jnp.concatenate(g_queries + g_keys + g_values, 1)
    acc[:, QKV : QKV + 3 * D] += dot_tn(in_one, g_projected)
    send(QKV, WIDE, 1)
    bias_acc[:, QKV : QKV + 3 * D] += col_sum(g_projected.astype(jnp.float32))
    g_in_one = dot_nt(g_projected, wqkv[...])
    gmod_ref[0, 1:2] = col_sum(g_in_one * norm_one)
    gmod_ref[0, 0:1] = col_sum(g_in_one)
    g_tokens = (g_residual + norm_back(g_in_one * scale_one, norm_one, rstd_one)).astype(jnp.bfloat16)
    for p in range(parts):
        outs[p][1, 0] = g_tokens[p * rows : (p + 1) * rows]

    @pl.when(step == steps - 1)
    def _():
        for copy in sent(UP, QKV, 0) + sent(QKV, WIDE, 1):
            copy.wait()


def layer_call(bit, live, blocks, mod, weights, carried, buffers, place, size, last, room):
    parts = len(blocks)
    images, rows = blocks[0].shape[1:3]
    first = carried is None
    resident = [pl.BlockSpec(w.shape, lambda i: (0, 0), pipeline_mode=pl.Buffered(1)) for w in weights]
    block_spec = pl.BlockSpec((2, 1, rows, D), lambda i: (0, i, 0, 0))
    out_spec = pl.BlockSpec((2, 1, rows, D), lambda i: (0, i + place, 0, 0))
    mod_spec = pl.BlockSpec((1, 6, D), lambda i: (i, 0, 0))
    any_spec = pl.BlockSpec(memory_space=pl.ANY)
    bias_spec = pl.BlockSpec((1, WIDE), lambda i: (0, 0))
    in_specs = (
        [pl.BlockSpec(memory_space=pltpu.SMEM)] * 2 + [block_spec] * parts + [mod_spec] + resident
    )
    args = [bit.reshape(1), live, *blocks, mod, *weights]
    aliases = {}
    if not first:
        in_specs += [any_spec, bias_spec]
        if not last:
            aliases[len(args)] = parts + 2
        args += list(carried)
    if buffers is not None:
        in_specs += [any_spec] * parts
        aliases.update({len(args) + p: p for p in range(parts)})
        args += list(buffers)
    if last:
        sums = [jax.ShapeDtypeStruct((D // 2, WIDE), jnp.bfloat16)] * 2
        sums += [jax.ShapeDtypeStruct((room, rows, D), jnp.bfloat16)] * 2
    else:
        sums = [jax.ShapeDtypeStruct((D, WIDE), jnp.float32)]
    scratch = [
        pltpu.VMEM((D, WIDE), jnp.float32),
        pltpu.VMEM((HEADS, parts * rows, parts * rows), jnp.float32),
        pltpu.SemaphoreType.DMA((4,)),
    ]
    if last:
        scratch.append(pltpu.VMEM((D, WIDE), jnp.bfloat16))
    result = pl.pallas_call(
        functools.partial(layer_kernel, parts, first, last, buffers is not None),
        grid=(images,),
        in_specs=in_specs,
        out_specs=[out_spec] * parts + [mod_spec, bias_spec] + [any_spec] * len(sums),
        out_shape=[jax.ShapeDtypeStruct((2, size, rows, D), jnp.bfloat16)] * parts
        + [
            jax.ShapeDtypeStruct((images, 6, D), jnp.float32),
            jax.ShapeDtypeStruct((1, WIDE), jnp.float32),
        ]
        + sums,
        scratch_shapes=scratch,
        input_output_aliases=aliases,
        cost_estimate=pl.CostEstimate(
            flops=KERNEL_FLOPS * images, transcendentals=0, bytes_accessed=8 * images * parts * rows * D
        ),
        compiler_params=pltpu.CompilerParams(vmem_limit_bytes=52 * 1024 * 1024),
    )(*args)
    return result[:parts], result[parts], (*result[parts + 2 :], result[parts + 1])


def finish_kernel(bit_ref, mine_ref, other_ref, up_ref, down_ref, qkv_ref, out_ref):
    low = bit_ref[0] == 0
    size = mine_ref.shape[0]
    mine, other = mine_ref[...], other_ref[...]
    down = []
    for k in range(2):
        part = jnp.where(low, mine, other) if k == 0 else jnp.where(low, other, mine)
        span = slice(k * size, (k + 1) * size)
        up_ref[span] = part[:, UP : UP + FF].astype(jnp.float32)
        qkv_ref[span] = part[:, QKV : QKV + 3 * D].astype(jnp.float32)
        out_ref[span] = part[:, OUT : OUT + D].astype(jnp.float32)
        down.append(part[:, DOWN : DOWN + FF])
    down_ref[...] = jnp.concatenate(down, 0).T.astype(jnp.float32)


def finish(bit, mine, other):
    full = pl.BlockSpec(memory_space=pltpu.VMEM)
    rows = 2 * mine.shape[0]
    shapes = [(rows, FF), (FF, rows), (rows, 3 * D), (rows, D)]
    return pl.pallas_call(
        finish_kernel,
        in_specs=[pl.BlockSpec(memory_space=pltpu.SMEM), full, full],
        out_specs=[full] * 4,
        out_shape=[jax.ShapeDtypeStruct(shape, jnp.float32) for shape in shapes],
        compiler_params=pltpu.CompilerParams(vmem_limit_bytes=52 * 1024 * 1024),
    )(bit.reshape(1), mine, other)


def ada_kernel(small_ref, weight_ref, grad_ref, bias_ref, side_ref, cond_out, level_ref):
    rows = small_ref.shape[0]
    small = small_ref[:, : 6 * D]
    slot = lax.broadcasted_iota(jnp.int32, (side_ref.shape[0], rows), 0)
    row = lax.broadcasted_iota(jnp.int32, (side_ref.shape[0], rows), 1)
    picks = (row % side_ref.shape[0] == slot).astype(jnp.bfloat16)
    bias_ref[...] = col_sum(dot_nn(picks, small))
    side_ref[...] = dot_nn(picks, small_ref[:, 6 * D : COND])
    cond = small_ref[:, COND : COND + D].astype(jnp.float32) + small_ref[:, COND + D : LEVEL].astype(jnp.float32)
    gate = jax.nn.sigmoid(cond)
    g_cond = dot_nt(small, weight_ref[...]) * (gate * (1.0 + cond * (1.0 - gate)))
    cond_out[...] = g_cond
    levels = small_ref[:, LEVEL : LEVEL + 128].astype(jnp.float32)
    onehot = (levels == lax.broadcasted_iota(jnp.int32, (rows, 128), 1).astype(jnp.float32)).astype(jnp.float32)
    level_ref[...] = lax.dot_general(
        onehot, g_cond, (((0,), (0,)), ((), ())), precision=highest, preferred_element_type=jnp.float32
    )[:LEVELS]
    grad_ref[...] = dot_tn((cond * gate).astype(jnp.bfloat16), small)


def ada_call(small, weight, own):
    full = pl.BlockSpec(memory_space=pltpu.VMEM)
    rows = small.shape[0]
    shapes = [(D, 6 * D), (1, 6 * D), (own, SIDE), (rows, D), (LEVELS, D)]
    return pl.pallas_call(
        ada_kernel,
        in_specs=[full] * 2,
        out_specs=[full] * 5,
        out_shape=[jax.ShapeDtypeStruct(shape, jnp.float32) for shape in shapes],
        cost_estimate=pl.CostEstimate(flops=6_000_000_000, transcendentals=0, bytes_accessed=8_000_000),
        compiler_params=pltpu.CompilerParams(vmem_limit_bytes=52 * 1024 * 1024),
    )(small, weight)


def cut(array, start, size, axis=0):
    return lax.dynamic_slice_in_dim(array, start, size, axis)


def group_stages(size):
    bits = [1 << k for k in range(size.bit_length() - 1)]
    if size == 8:
        table = [[1] * 8, [2 if i % 2 == 0 else 4 for i in range(8)], [4 if i % 2 == 0 else 2 for i in range(8)]]
    else:
        table = [[bit] * size for bit in bits]
    return table


def stage_bit(stage, index):
    masks = jnp.asarray(stage, jnp.int32)[index] if len(set(stage)) > 1 else stage[0]
    return jnp.where((index & masks) != 0, 1, 0)


def swap(array, stage):
    return lax.ppermute(array, "grp", [(i, i ^ bit) for i, bit in enumerate(stage)])


def seq_shift(array, shift, size):
    return lax.ppermute(array, "seq", [(i, (i + shift) % size) for i in range(size)])


def scatter_grp(keep, give, index, stages, after):
    given = []
    for k, stage in enumerate(stages):
        if k in after:
            give = tied(give, after[k])
        given.append(give)
        got = swap(give, stage)
        if k + 1 < len(stages):
            size = keep.shape[0] // 2
            bit = stage_bit(stages[k + 1], index)
            keep, give = [
                (cut(keep, b * size, size).astype(jnp.float32) + cut(got, b * size, size).astype(jnp.float32)).astype(
                    jnp.bfloat16
                )
                for b in (bit, 1 - bit)
            ]
    return (keep.astype(jnp.float32) + got.astype(jnp.float32)).astype(jnp.bfloat16), given


def scatter_seq(array, place, seq):
    size = array.shape[1] // seq
    total = cut(array, place * size, size, 1).astype(jnp.float32)
    for shift in seq_shifts(seq)[1:]:
        total = total + seq_shift(cut(array, ((place + shift) % seq) * size, size, 1), shift, seq).astype(jnp.float32)
    return total.astype(jnp.bfloat16)


def gather_seq(array, place, seq, axis):
    size = array.shape[axis]
    shape = list(array.shape)
    shape[axis] = size * seq
    whole = lax.dynamic_update_slice_in_dim(jnp.zeros(shape, array.dtype), array, place * size, axis)
    for shift in seq_shifts(seq)[1:]:
        got = seq_shift(array, shift, seq)
        whole = lax.dynamic_update_slice_in_dim(whole, got, ((place - shift) % seq) * size, axis)
    return whole


def join(array, index, stage):
    got = swap(array, stage)
    low = stage_bit(stage, index) == 0
    return jnp.where(low, jnp.concatenate([array, got], 0), jnp.concatenate([got, array], 0))


def join_seq(array, place, bit, seq):
    got = lax.ppermute(array, "seq", [(i, i ^ bit) for i in range(seq)])
    low = (place & bit) == 0
    return jnp.where(low, jnp.concatenate([array, got], 0), jnp.concatenate([got, array], 0))


def join_last(array, index, stage):
    got = swap(array, stage)
    low = stage_bit(stage, index) == 0
    first, second = jnp.where(low, array, got), jnp.where(low, got, array)
    half = first.shape[0] // 2
    odd = (index & 1) == 0
    return jnp.concatenate(
        [
            first[:half],
            jnp.where(odd, second[:half], first[half:]),
            jnp.where(odd, first[half:], second[:half]),
            second[half:],
        ],
        0,
    )


def group_steps(index, group):
    stages = group_stages(group)
    if group == 8:
        stages[1:] = stages[:0:-1]
    steps = [functools.partial(join, index=index, stage=stage) for stage in stages]
    if group == 8:
        steps[-1] = functools.partial(join_last, index=index, stage=stages[-1])
    return steps


def seq_shifts(seq):
    return (0, 2, 1, 3) if seq == 4 else tuple(range(seq))


def tied(values, after):
    return lax.optimization_barrier((values, after))[0]


def level_rows(levels):
    return (levels[:, None] == jnp.arange(LEVELS, dtype=levels.dtype)[None, :]).astype(jnp.float32)


def shards(
    group,
    seq,
    tokens,
    cotangent,
    condition,
    mask_flags,
    noise_levels,
    level_table,
    ada_weight,
    ada_bias,
    qkv_weight,
    query_value_bias,
    output_weight,
    output_bias,
    up_weight,
    up_bias,
    down_weight,
    down_bias,
):
    batches, images, rows = tokens.shape[:3]
    count = batches * images
    own = count // seq
    place = lax.axis_index("seq")
    index = lax.axis_index("grp")
    stages = group_stages(group)
    shifts = seq_shifts(seq)
    chunks = CHUNKS if sum(CHUNKS) == own else (own,)
    starts = [sum(chunks[:c]) for c in range(len(chunks))]
    whole = (tokens.reshape(count, rows, D), cotangent.reshape(count, rows, D))
    condition = condition.reshape(count, D)
    noise_levels = noise_levels.reshape(count)

    def pieces(chunk):
        return [
            jnp.stack([cut(array, ((place + shift) % seq) * own + starts[chunk], chunks[chunk]) for array in whole])
            for shift in shifts
        ]

    def fetch(sources):
        return [block if shift == 0 else seq_shift(block, shift, seq) for shift, block in zip(shifts, sources)]

    blocks = fetch(pieces(0))
    later = [pieces(chunk) for chunk in range(1, len(chunks))]

    flags = cut(mask_flags.reshape(count), place * own, own)
    sources = jnp.stack([(place - shift) % seq for shift in shifts])
    live = jnp.logical_or(flags[:, None] == 0, sources[None, :] * rows < KEEP).astype(jnp.float32)

    mine = cut(condition, place * own, own) + jnp.dot(
        level_rows(cut(noise_levels, place * own, own)), level_table, precision=highest
    )
    modulation = (
        jnp.dot(jax.nn.silu(mine).astype(jnp.bfloat16), ada_weight, preferred_element_type=jnp.float32) + ada_bias
    ).reshape(own, 6, D)

    bias_full = jnp.concatenate([query_value_bias[:D], jnp.zeros((D,), jnp.float32), query_value_bias[D:]])
    weights = (
        qkv_weight,
        output_weight,
        up_weight,
        down_weight,
        bias_full[None],
        output_bias[None],
        up_bias[None],
        down_bias[None],
    )
    high = mine.astype(jnp.bfloat16)
    own_levels = cut(noise_levels, place * own, own).astype(jnp.bfloat16)
    side = jnp.concatenate(
        [high, (mine - high.astype(jnp.float32)).astype(jnp.bfloat16), jnp.broadcast_to(own_levels[:, None], (own, 128))],
        1,
    )
    bit = stage_bit(stages[0], index)
    carried = None
    g_mods = []

    def give(buffer, shift, start, after, source=None):
        if shift != 0:
            buffer = seq_shift(tied(buffer, after), -shift, seq)
        start = ((place + (shift if source is None else source)) % seq) * own + start
        for k in range(2):
            targets[k] = lax.dynamic_update_slice_in_dim(targets[k], buffer[k], start, 0)
        return buffer

    def back(buffers, k, after):
        return seq_shift(tied(buffers[k], after), -shifts[k], seq) if k else buffers[0]

    def put(buffer, k, chunk):
        for which in range(2):
            targets[which] = lax.dynamic_update_slice_in_dim(
                targets[which], buffer[which], ((place + shifts[k]) % seq) * own + starts[chunk], 0
            )

    held = []
    released = None
    for chunk in range(len(chunks)):
        final = chunk + 1 == len(chunks)
        if chunk == 0:
            live, later = lax.optimization_barrier((live, later))
        following = None if final else fetch(tied(later[chunk], blocks))
        span = slice(starts[chunk], starts[chunk] + chunks[chunk])
        if final:
            early = [[back(buffers, k, (blocks, released)) for k in range(len(shifts))] for buffers in held[:-1]]
            ahead = [back(buffers, 2, (blocks, released)) for buffers in held[-1:]]
        buffers, g_mod, carried = layer_call(
            bit, live[span], blocks, modulation[span], weights, carried, None, 0, chunks[chunk], final, count
        )
        held.append(buffers)
        released = g_mod
        g_mods.append(g_mod)
        blocks = following

    keep, send, *targets, bias_sums = carried
    send = tied(send, (early, ahead))
    for chunk, buffers in enumerate(early):
        for k, buffer in enumerate(buffers):
            put(buffer, k, chunk)
    after = {}
    if len(chunks) > 1:
        middle = [ahead[0] if k == 2 else back(held[-2], k, early) for k in range(len(shifts))]
        after = {len(stages): (middle[1], middle[3])}
        for k, buffer in enumerate(middle):
            put(buffer, k, len(chunks) - 2)
    part, given = scatter_grp(keep, send, index, stages, after)
    if len(stages) in after:
        part = tied(part, after[len(stages)])
    quarter = scatter_seq(part, place, seq)
    given += [part, quarter]
    part = gather_seq(quarter, place, seq, 1)
    bias_side = jnp.pad(bias_sums, ((0, 0), (0, own * SIDE - WIDE))).reshape(own, SIDE)
    small = jnp.concatenate(
        [jnp.concatenate([g.reshape(-1, 6 * D) for g in g_mods]).astype(jnp.bfloat16), bias_side.astype(jnp.bfloat16), side],
        1,
    )
    small = tied(small, given[1])
    given = iter([given[-2]] * (len(stages) - 1) + given[-1:])
    for k in range(seq.bit_length() - 1):
        small = join_seq(small, place, 1 << k, seq)
    for step in group_steps(index, group):
        small = step(tied(small, next(given, part)))
    grad_ada, grad_ada_bias, bias_side, g_cond, grad_level = ada_call(small, ada_weight, own)
    final_rows = [back(held[-1], k, part) for k in range(len(shifts))]
    joins = list(reversed(stages[1:]))
    for k, stage in enumerate(joins):
        if k + 1 == len(joins):
            part = tied(part, (final_rows[1], small))
        part = join(part, index, stage)
    part, grad_ada = lax.optimization_barrier((part, grad_ada))
    part = tied(part, final_rows[2:])
    other = swap(part, stages[0])
    for k, buffer in enumerate(final_rows):
        put(buffer, k, len(chunks) - 1)
    grad_up, grad_down, grad_qkv, grad_out = finish(bit, part, other)

    grad_ada_bias = grad_ada_bias[0]
    bias_all = bias_side.reshape(own * SIDE)
    grad_condition = cut(g_cond, index * count, count)
    return (
        targets[0].reshape(batches, images, rows, D),
        targets[1].reshape(batches, images, rows, D),
        grad_condition.reshape(batches, images, D),
        grad_level,
        grad_ada,
        grad_ada_bias,
        grad_qkv,
        jnp.concatenate([bias_all[QKV : QKV + D], bias_all[QKV + 2 * D : QKV + 3 * D]]),
        grad_out,
        bias_all[OUT : OUT + D],
        grad_up,
        bias_all[UP : UP + FF],
        grad_down,
        bias_all[DOWN : DOWN + D],
    )


def solution(mesh):
    rows = P(None, "grp", "seq", None)
    in_specs = (rows, rows, P(None, "grp", None), P(None, "grp"), P(None, "grp")) + (P(),) * 11
    out_specs = (rows, rows, P(None, "grp", None)) + (P(),) * 11
    body = functools.partial(shards, mesh.shape["grp"], mesh.shape["seq"])
    return jax.shard_map(body, mesh=mesh, in_specs=in_specs, out_specs=out_specs, check_vma=False)
```
